128 devices in a mesh: band: 8 (over x, y_lo), ga: 16 (over z, y_hi, core).
Axes of the slice: x: 4, y: 4 (y_hi: 2, y_lo: 2; y = y_hi * 2 + y_lo), z: 4, core: 2. Of those that a mesh axis runs over, the one named last changes fastest.
Arguments:
- psi: float32 [4096, 8192], P('band', 'ga'), may hold values from -6 to 6
- lower: float32 [4096, 4096], P('band', 'ga'), as said below
Outputs:
- orthonormal: float32 [4096, 8192], P('band', 'ga')
- block_intersection: float32 [4096, 512], P('band')
The draws below stay inside these ranges and needn't reach their ends.
Inputs may be any that keep to these rules, and one draw needn't show every extreme that they name: lower is lower triangular with its diagonal between 1 and 2.
All inputs are finite; a program needn't handle non-finite values.
Results may differ from the reference program's by a relative error of at most 0.00022.
Values sent between devices are 32-bit elements; how exact they have to be, the bound alone decides.
A program may use at most 64 MiB of HBM per device.

```python
import math
import jax
import jax.numpy as jnp
from jax import lax

NB = 4096
NG = 8192
N_BAND = 8


def draw_lower(key, part):
    first, second = jax.random.split(jax.random.fold_in(key, 11))
    spread = jax.random.normal(first, (NB, NB), jnp.float32) * (2.0 / math.sqrt(NB))
    middle = jax.random.uniform(second, (NB,), jnp.float32, 1.0, 2.0)
    rowpos = lax.broadcasted_iota(jnp.int32, (NB, NB), 0)
    colpos = lax.broadcasted_iota(jnp.int32, (NB, NB), 1)
    return jnp.where(rowpos > colpos, spread, 0.0) + jnp.diag(middle)


def shard_levels(stream_key, extent, pieces, smallest, largest):
    def one(dim, shards_of):
        heights = jax.random.uniform(jax.random.fold_in(jax.random.fold_in(stream_key, 6), dim), (shards_of,), jnp.float32, smallest / len(pieces), largest / len(pieces))
        return jnp.repeat(jnp.exp(heights), extent[dim] // shards_of).reshape((-1,) + (1,) * (len(extent) - dim - 1))

    level = one(*pieces[0])
    for cut in pieces[1:]:
        level = level * one(*cut)
    return level


def bell_draw(key, extent, deviation, bound, shards=(), kind=jnp.bfloat16):
    array = deviation * jax.random.normal(key, extent, jnp.float32)
    if shards:
        array = array * shard_levels(key, extent, shards, -0.22, 0.18)
    return jnp.clip(array, -bound, bound).astype(kind)


def setup_inputs(seed: int = 0) -> dict:
    splits = jax.random.split(jax.random.key(seed), 3)
    psi = bell_draw(splits[0], (NB, NG), 1.0, 6.0, ((0, 8), (1, 16)), jnp.float32)
    lower = draw_lower(jax.random.fold_in(splits[2], 71), 0)
    return {"psi": psi, "lower": lower}


def reference(psi, lower):
    solved = jax.scipy.linalg.solve_triangular(lower, psi, lower=True)
    blocks = solved.reshape(N_BAND, NB // N_BAND, NG)
    intersection = jnp.einsum('bik,bjk->bij', blocks, blocks, precision=lax.Precision.HIGHEST) / NG
    return (solved, intersection.reshape(NB, NB // N_BAND))
```

```python
import jax
import jax.numpy as jnp
from jax import lax
from jax.experimental import pallas as pl
from jax.experimental.pallas import tpu as pltpu
from jax.sharding import PartitionSpec as P

MESH = pl.DeviceIdType.MESH
F32 = jnp.float32
BF16 = jnp.bfloat16
NG = 8192


def split(a):
    high = a.astype(BF16)
    return high, (a - high.astype(F32)).astype(BF16)


def product(a, b, dims=(((1,), (0,)), ((), ()))):
    ah, al = split(a)
    bh, bl = split(b)

    def dot(p, q):
        return lax.dot_general(p, q, dims, preferred_element_type=F32)

    return dot(ah, bh) + (dot(ah, bl) + dot(al, bh))


def kernel(
    psi, lower, out, inter,
    tiles, ys, rhs, owned, part, half, pieces, whole, inverse,
    tile_sem, ring_sem, cross_sem, pair_sem, swap_sem, rhs_sem, rhs_send,
    y_sem, y_send, own_sem, own_send, half_sem, rs_sem, rs_send, ag_sem, ag_send,
    ag_cross, local_sem,
):
    band = lax.axis_index("band")
    ga = lax.axis_index("ga")
    x, y_lo = band // 2, band % 2
    z, y_hi, c = ga // 4, (ga // 2) % 2, ga % 2
    y = 2 * y_hi + y_lo
    h_own = x // 2
    outer = jnp.logical_or(x == 0, x == 3)
    x_low = jnp.minimum(x, 3 - x)
    place = 2 * h_own + y_lo

    def device(dx, dy, dz, dc):
        return (2 * dx + dy % 2, 4 * dz + 2 * (dy // 2) + dc)

    def xs(h):
        return x_low if h == 0 else 3 - x_low

    def slot(row, j, a, b):
        return ((row * 8 + j) * 2 + a) * 2 + b

    pending = []

    def send(cond, src, dst, s_sem, r_sem, target, later=True):
        copy = pltpu.make_async_remote_copy(
            src_ref=src, dst_ref=dst, send_sem=s_sem, recv_sem=r_sem,
            device_id=target, device_id_type=MESH,
        )
        if cond is None:
            copy.start()
        else:
            pl.when(cond)(copy.start)
        if later:
            pending.append((cond, copy))
        return copy

    def arrived(ref, sem):
        pltpu.make_async_copy(ref, ref, sem).wait()

    psi_here = pltpu.make_async_copy(
        psi.at[:, pl.ds(pl.multiple_of(128 * place, 128), 128)], rhs.at[place], local_sem.at[0]
    )
    psi_here.start()

    j_own = 2 * z + y_hi
    loads = []
    for a in range(2):
        load = pltpu.make_async_copy(
            lower.at[256 * a : 256 * a + 256, :], tiles.at[slot(place, j_own, a, c)],
            local_sem.at[1 + a],
        )
        load.start()
        loads.append(load)

    for q in range(4):
        send(
            place != q,
            psi.at[:, 128 * q : 128 * q + 128], rhs.at[place],
            rhs_send.at[q], rhs_sem.at[place],
            device(xs(q // 2), 2 * y_hi + q % 2, z, c),
        )
    for load in loads:
        load.wait()

    @pl.when(j_own == band)
    def _():
        where = slot(place, j_own, c, c)
        rows = lax.broadcasted_iota(jnp.int32, (256, 256), 0)
        cols = lax.broadcasted_iota(jnp.int32, (256, 256), 1)
        tri = tiles[where]
        diag = jnp.where(rows == cols, tri, 0.0)
        down = 1.0 / jnp.sum(diag, axis=1, keepdims=True)
        across = 1.0 / jnp.sum(diag, axis=0, keepdims=True)
        pairs = jnp.logical_and(rows == cols + 1, rows % 2 == 1)
        inverse[...] = jnp.where(rows == cols, down, 0.0) - jnp.where(
            pairs, tri * down * across, 0.0
        )

        def level(k, carry):
            rk, ck = rows >> k, cols >> k
            inside = jnp.logical_and(rk == ck + 1, rk % 2 == 1)
            below = jnp.where(inside, tiles[where], 0.0)
            now = inverse[...]
            inverse[...] = now - product(now, product(below, now))
            return carry

        lax.fori_loop(1, 8, level, 0)
        tiles[where] = inverse[...]

    def place_of(v):
        return lax.rem(v + 8, 4)

    def event(h, a, k, s):
        sgn = 1 - 2 * a
        yo = place_of(y - sgn * (k * c + s * (1 - c)))
        zo = place_of(z - sgn * (k * (1 - c) + s * c))
        row, j = 2 * h + yo % 2, 2 * zo + yo // 2
        i = 2 * xs(h) + yo % 2
        here = slot(row, j, a, c)
        real = 2 * j + c <= 2 * i + a
        ref = tiles.at[here]
        if k or s:
            pl.when(real)(lambda: arrived(ref, tile_sem.at[here]))
        else:
            mine = h_own == h
            pl.when(jnp.logical_and(real, jnp.logical_not(mine)))(
                lambda: arrived(ref, tile_sem.at[here])
            )
        first = device(x, place_of(y + sgn * c), place_of(z + sgn * (1 - c)), c)
        second = device(x, place_of(y + sgn * (1 - c)), place_of(z + sgn * c), c)
        if s == 0 and k < 3:
            send(real, ref, ref, ring_sem.at[(h * 2 + a) * 3 + k], tile_sem.at[here], first)
        if s < 3:
            send(real, ref, ref, cross_sem.at[((h * 2 + a) * 4 + k) * 3 + s],
                 tile_sem.at[here], second)
        send(real, ref, ref, pair_sem.at[((h * 2 + a) * 4 + k) * 4 + s], tile_sem.at[here],
             device(x, y, z, 1 - c))

    for a in range(2):
        here = slot(place, j_own, a, c)
        send(2 * j_own + c <= 2 * band + a, tiles.at[here], tiles.at[here], swap_sem.at[a],
             tile_sem.at[here], device(3 - x, y, z, c))

    def line(h):
        for k in range(4):
            for a in range(2):
                event(h, a, k, 0)

    def across(h, s):
        for k in range(4):
            for a in range(2):
                event(h, a, k, s)

    def tile(row, j, a, b):
        return tiles[slot(row, j, a, b)]

    def from_sibling(row, j, a):
        here = slot(row, j, a, 1 - c)
        arrived(tiles.at[here], tile_sem.at[here])

    def update(row, j):
        for a in range(2):
            from_sibling(row, j, a)
        top, bottom = ys[2 * j], ys[2 * j + 1]
        for a in range(2):
            rhs[row, 256 * a : 256 * a + 256, :] = rhs[row, 256 * a : 256 * a + 256, :] - (
                product(tile(row, j, a, 0), top) + product(tile(row, j, a, 1), bottom)
            )

    def solve(row, i):
        @pl.when(c == 0)
        def _():
            from_sibling(row, i, 1)

        @pl.when(c == 1)
        def _():
            from_sibling(row, i, 0)
            from_sibling(row, i, 1)

        top = product(tile(row, i, 0, 0), rhs[row, 0:256, :])
        ys[2 * i] = top
        bottom = product(
            tile(row, i, 1, 1), rhs[row, 256:512, :] - product(tile(row, i, 1, 0), top)
        )
        ys[2 * i + 1] = bottom

    def deliver(h, r, later):
        row = 2 * h + r
        i = 2 * xs(h) + r
        block = ys.at[pl.ds(2 * i, 2)]
        send(None if h == 0 else jnp.logical_not(outer), block, block, y_send.at[row],
             y_sem.at[i], device(x + 1 - 2 * (x % 2), y, z, c), later)
        send(place != row, block, owned.at[place], own_send.at[row], own_sem.at[place],
             device(xs(h), 2 * y_hi + r, z, c), later)

    def stage(h, later):
        count = 2 * xs(h)
        for r in range(2):
            row = 2 * h + r

            @pl.when(place != row)
            def _():
                arrived(rhs.at[row], rhs_sem.at[row])

            @pl.when(place == row)
            def _():
                psi_here.wait()

        def step(j, carry):
            there = jnp.logical_not(outer) if h == 0 else jnp.logical_and(outer, j >= 2)

            @pl.when(there)
            def _():
                arrived(ys.at[pl.ds(2 * j, 2)], y_sem.at[j])

            update(2 * h, j)
            update(2 * h + 1, j)
            return carry

        lax.fori_loop(0, count, step, 0)
        for r in range(2):
            if r:
                update(2 * h + 1, count)
            solve(2 * h + r, count + r)
            deliver(h, r, later)

            @pl.when(place == 2 * h + r)
            def _():
                i = count + r
                owned[2 * h + r, 0] = ys[2 * i]
                owned[2 * h + r, 1] = ys[2 * i + 1]

    line(0)
    for s in range(1, 4):
        across(0, s)
    line(1)

    @pl.when(outer)
    def _():
        stage(0, False)

    across(1, 1)
    across(1, 2)

    @pl.when(jnp.logical_not(outer))
    def _():
        stage(0, False)

    across(1, 3)
    stage(1, True)

    writes = []
    for q in range(4):
        @pl.when(place != q)
        def _():
            arrived(owned.at[q], own_sem.at[q])

        for a in range(2):
            write = pltpu.make_async_copy(
                owned.at[q, a], out.at[256 * a : 256 * a + 256, 128 * q : 128 * q + 128],
                local_sem.at[3 + 2 * q + a],
            )
            write.start()
            writes.append(write)
        block = owned[q].reshape(512, 128)
        term = product(block, block, (((1,), (1,)), ((), ())))
        if q == 0:
            part[...] = term
        else:
            part[...] = part[...] + term

    lines = pl.ds(pl.multiple_of(256 * c, 256), 256)
    other = pl.ds(pl.multiple_of(256 - 256 * c, 256), 256)
    send(None, part.at[other], half, half_sem.at[0], half_sem.at[1], device(x, y, z, 1 - c))
    arrived(half, half_sem.at[1])
    half[...] = half[...] + part[lines, :]
    m = 2 * z + y_hi
    for t in range(1, 8):
        to = lax.rem(m + t, 8)
        send(None, half.at[pl.ds(pl.multiple_of(32 * to, 32), 32)], pieces.at[t - 1],
             rs_send.at[t - 1], rs_sem.at[t - 1],
             device(x, 2 * (to % 2) + y_lo, to // 2, c))
    total = half[pl.ds(pl.multiple_of(32 * m, 32), 32), :]
    for t in range(1, 8):
        arrived(pieces.at[t - 1], rs_sem.at[t - 1])
        total = total + pieces[t - 1]
    mine = c * 8 + m
    whole[mine] = total * (1.0 / NG)
    for t in range(1, 8):
        to = lax.rem(m + t, 8)
        send(None, whole.at[mine], whole.at[mine], ag_send.at[t - 1], ag_sem.at[mine],
             device(x, 2 * (to % 2) + y_lo, to // 2, c))
    send(None, whole.at[mine], whole.at[mine], ag_cross.at[0], ag_sem.at[mine],
         device(x, y, z, 1 - c))
    for t in range(1, 8):
        at = c * 8 + lax.rem(m + 8 - t, 8)
        arrived(whole.at[at], ag_sem.at[at])
        send(None, whole.at[at], whole.at[at], ag_cross.at[t], ag_sem.at[at],
             device(x, y, z, 1 - c))
    for t in range(8):
        at = (1 - c) * 8 + t
        arrived(whole.at[at], ag_sem.at[at])
    final = pltpu.make_async_copy(whole, inter, local_sem.at[11])
    final.start()
    for cond, copy in pending:
        if cond is None:
            copy.wait_send()
        else:
            pl.when(cond)(copy.wait_send)
    for row in range(2):
        i = 2 * xs(0) + row
        block = ys.at[pl.ds(2 * i, 2)]
        arrived(block, y_send.at[row])

        @pl.when(place != row)
        def _():
            arrived(block, own_send.at[row])

    for write in writes:
        write.wait()
    final.wait()


def local(psi, lower):
    dma = pltpu.SemaphoreType.DMA
    out, inter = pl.pallas_call(
        kernel,
        out_shape=(
            jax.ShapeDtypeStruct((512, 512), F32),
            jax.ShapeDtypeStruct((16, 32, 512), F32),
        ),
        in_specs=[pl.BlockSpec(memory_space=pl.ANY)] * 2,
        out_specs=(pl.BlockSpec(memory_space=pl.ANY),) * 2,
        scratch_shapes=[
            pltpu.VMEM((128, 256, 256), F32),
            pltpu.VMEM((16, 256, 128), F32),
            pltpu.VMEM((4, 512, 128), F32),
            pltpu.VMEM((4, 2, 256, 128), F32),
            pltpu.VMEM((512, 512), F32),
            pltpu.VMEM((256, 512), F32),
            pltpu.VMEM((7, 32, 512), F32),
            pltpu.VMEM((16, 32, 512), F32),
            pltpu.VMEM((256, 256), F32),
            dma((128,)), dma((12,)), dma((48,)), dma((64,)), dma((2,)), dma((4,)), dma((4,)),
            dma((8,)), dma((4,)), dma((4,)), dma((4,)), dma((2,)), dma((7,)), dma((7,)),
            dma((16,)), dma((7,)), dma((8,)), dma((12,)),
        ],
        compiler_params=pltpu.CompilerParams(
            has_side_effects=True, vmem_limit_bytes=60 * 1024 * 1024
        ),
    )(psi, lower)
    return out, inter.reshape(512, 512)


def solution(mesh):
    return jax.shard_map(
        local,
        mesh=mesh,
        in_specs=(P("band", "ga"), P("band", "ga")),
        out_specs=(P("band", "ga"), P("band", None)),
        check_vma=False,
    )
```

```python
import jax
import jax.numpy as jnp
from jax import lax
from jax.experimental import pallas as pl
from jax.experimental.pallas import tpu as pltpu
from jax.sharding import PartitionSpec as P

MESH = pl.DeviceIdType.MESH
F32 = jnp.float32
BF16 = jnp.bfloat16
NG = 8192


def split(a):
    high = a.astype(BF16)
    return high, (a - high.astype(F32)).astype(BF16)


def product(a, b, dims=(((1,), (0,)), ((), ()))):
    ah, al = split(a)
    bh, bl = split(b)

    def dot(p, q):
        return lax.dot_general(p, q, dims, preferred_element_type=F32)

    return dot(ah, bh) + (dot(ah, bl) + dot(al, bh))


def kernel(
    psi, lower, out, inter,
    tiles, ys, rhs, owned, part, half, pieces, whole, inverse,
    tile_sem, ring_sem, cross_sem, pair_sem, swap_sem, rhs_sem, rhs_send,
    y_sem, y_send, own_sem, own_send, half_sem, rs_sem, rs_send, ag_sem, ag_send,
    ag_cross, local_sem,
):
    band = lax.axis_index("band")
    ga = lax.axis_index("ga")
    x, y_lo = band // 2, band % 2
    z, y_hi, c = ga // 4, (ga // 2) % 2, ga % 2
    y = 2 * y_hi + y_lo
    h_own = x // 2
    outer = jnp.logical_or(x == 0, x == 3)
    x_low = jnp.minimum(x, 3 - x)
    place = 2 * h_own + y_lo

    def device(dx, dy, dz, dc):
        return (2 * dx + dy % 2, 4 * dz + 2 * (dy // 2) + dc)

    def xs(h):
        return x_low * (1 - h) + (3 - x_low) * h

    def slot(row, j, a, b):
        return ((row * 8 + j) * 2 + a) * 2 + b

    pending = []

    def send(cond, src, dst, s_sem, r_sem, target, later=True):
        copy = pltpu.make_async_remote_copy(
            src_ref=src, dst_ref=dst, send_sem=s_sem, recv_sem=r_sem,
            device_id=target, device_id_type=MESH,
        )
        if cond is None:
            copy.start()
        else:
            pl.when(cond)(copy.start)
        if later:
            pending.append((cond, copy))
        return copy

    def arrived(ref, sem):
        pltpu.make_async_copy(ref, ref, sem).wait()

    j_own = 2 * z + y_hi
    loads = []
    for a in range(2):
        load = pltpu.make_async_copy(
            lower.at[256 * a : 256 * a + 256, :], tiles.at[slot(place, j_own, a, c)],
            local_sem.at[1 + a],
        )
        load.start()
        loads.append(load)
    psi_here = pltpu.make_async_copy(
        psi.at[:, pl.ds(pl.multiple_of(128 * place, 128), 128)], rhs.at[place], local_sem.at[0]
    )
    psi_here.start()

    def place_of(v):
        return lax.rem(v + 8, 4)

    barrier = pltpu.get_barrier_semaphore()
    friends = [
        (3 - x, y, z, c), (x, 2 * y_hi + 1 - y_lo, z, c), (3 - x, 2 * y_hi + 1 - y_lo, z, c),
        (x + 1 - 2 * (x % 2), y, z, c), (x, y, z, 1 - c),
        (x, place_of(y + 1), z, c), (x, place_of(y - 1), z, c),
        (x, y, place_of(z + 1), c), (x, y, place_of(z - 1), c),
    ] + [
        (x, 2 * (lax.rem(j_own + t, 8) % 2) + y_lo, lax.rem(j_own + t, 8) // 2, c)
        for t in range(1, 8)
    ]
    for friend in friends:
        pl.semaphore_signal(barrier, inc=1, device_id=device(*friend), device_id_type=MESH)
    pl.semaphore_wait(barrier, len(friends))
    for load in loads:
        load.wait()

    def quarter(h, a, k, s):
        sgn = 1 - 2 * a
        yo = place_of(y - sgn * (k * c + s * (1 - c)))
        zo = place_of(z - sgn * (k * (1 - c) + s * c))
        row, j = 2 * h + yo % 2, 2 * zo + yo // 2
        i = 2 * xs(h) + yo % 2
        here = slot(row, j, a, c)
        return here, 2 * j + c <= 2 * i + a

    def await_quarter(h, a, k, s):
        here, real = quarter(h, a, k, s)
        pl.when(real)(lambda: arrived(tiles.at[here], tile_sem.at[here]))

    def along(h, a, k, also=None):
        here, real = quarter(h, a, k, 0)
        sgn = 1 - 2 * a
        cond = real if also is None else jnp.logical_and(real, also)
        ref = tiles.at[here]
        send(cond, ref, ref, ring_sem.at[(h * 2 + a) * 3 + k], tile_sem.at[here],
             device(x, place_of(y + sgn * c), place_of(z + sgn * (1 - c)), c))

    def over(h, a, k, s, also=None):
        here, real = quarter(h, a, k, s)
        sgn = 1 - 2 * a
        cond = real if also is None else jnp.logical_and(real, also)
        ref = tiles.at[here]
        send(cond, ref, ref, cross_sem.at[((h * 2 + a) * 4 + k) * 3 + s], tile_sem.at[here],
             device(x, place_of(y + sgn * (1 - c)), place_of(z + sgn * c), c))

    def to_sibling(h, a, k, s, also=None):
        here, real = quarter(h, a, k, s)
        cond = real if also is None else jnp.logical_and(real, also)
        ref = tiles.at[here]
        send(cond, ref, ref, pair_sem.at[((h * 2 + a) * 4 + k) * 4 + s], tile_sem.at[here],
             device(x, y, z, 1 - c))

    h_other = 1 - h_own
    diagonal = j_own == band

    def own_quarters(ready):
        for a in range(2):
            here, real = quarter(h_own, a, 0, 0)
            send(jnp.logical_and(real, ready(a)), tiles.at[here], tiles.at[here],
                 swap_sem.at[a], tile_sem.at[here], device(3 - x, y, z, c), False)
        for a in range(2):
            along(h_own, a, 0, ready(a))
        for a in range(2):
            over(h_own, a, 0, 0, jnp.logical_and(ready(a), h_own == 0))
            to_sibling(h_own, a, 0, 0, ready(a))

    def send_later():
        for a in range(2):
            here, real = quarter(h_own, a, 0, 0)
            pl.when(real)(lambda: arrived(tiles.at[here], swap_sem.at[a]))

    own_quarters(lambda a: jnp.logical_not(jnp.logical_and(diagonal, c == a)))

    @pl.when(diagonal)
    def _():
        where = slot(place, j_own, c, c)
        rows = lax.broadcasted_iota(jnp.int32, (256, 256), 0)
        cols = lax.broadcasted_iota(jnp.int32, (256, 256), 1)
        tri = tiles[where]
        diag = jnp.where(rows == cols, tri, 0.0)
        down = 1.0 / jnp.sum(diag, axis=1, keepdims=True)
        across = 1.0 / jnp.sum(diag, axis=0, keepdims=True)
        pairs = jnp.logical_and(rows == cols + 1, rows % 2 == 1)
        inverse[...] = jnp.where(rows == cols, down, 0.0) - jnp.where(
            pairs, tri * down * across, 0.0
        )

        def level(k, carry):
            rk, ck = rows >> k, cols >> k
            inside = jnp.logical_and(rk == ck + 1, rk % 2 == 1)
            below = jnp.where(inside, tiles[where], 0.0)
            now = inverse[...]
            inverse[...] = now - product(now, product(below, now))
            return carry

        lax.fori_loop(1, 8, level, 0)
        tiles[where] = inverse[...]

    own_quarters(lambda a: jnp.logical_and(diagonal, c == a))

    for q in range(4):
        send(
            place != q,
            psi.at[:, 128 * q : 128 * q + 128], rhs.at[place],
            rhs_send.at[q], rhs_sem.at[place],
            device(xs(q // 2), 2 * y_hi + q % 2, z, c),
        )

    def line(h, k):
        for a in range(2):
            await_quarter(h, a, k, 0)
            if k < 3:
                along(h, a, k)
            over(h, a, k, 0, h == 0)
            to_sibling(h, a, k, 0)

    def across(h, s):
        for k in range(4):
            for a in range(2):
                await_quarter(h, a, k, s)
                if s < 3:
                    over(h, a, k, s)
                to_sibling(h, a, k, s)

    def tile(row, j, a, b):
        return tiles[slot(row, j, a, b)]

    def from_sibling(row, j, a):
        here = slot(row, j, a, 1 - c)
        arrived(tiles.at[here], tile_sem.at[here])

    def update(row, j):
        for a in range(2):
            from_sibling(row, j, a)
        top, bottom = ys[2 * j], ys[2 * j + 1]
        for a in range(2):
            rhs[row, 256 * a : 256 * a + 256, :] = rhs[row, 256 * a : 256 * a + 256, :] - (
                product(tile(row, j, a, 0), top) + product(tile(row, j, a, 1), bottom)
            )

    def solve(row, i):
        @pl.when(c == 0)
        def _():
            from_sibling(row, i, 1)

        @pl.when(c == 1)
        def _():
            from_sibling(row, i, 0)
            from_sibling(row, i, 1)

        top = product(tile(row, i, 0, 0), rhs[row, 0:256, :])
        ys[2 * i] = top
        bottom = product(
            tile(row, i, 1, 1), rhs[row, 256:512, :] - product(tile(row, i, 1, 0), top)
        )
        ys[2 * i + 1] = bottom

    def deliver(h, r):
        row = 2 * h + r
        i = 2 * xs(h) + r
        block = ys.at[pl.ds(2 * i, 2)]
        send(None if h == 0 else jnp.logical_not(outer), block, block, y_send.at[row],
             y_sem.at[i], device(x + 1 - 2 * (x % 2), y, z, c), False)
        send(place != row, block, owned.at[place], own_send.at[row], own_sem.at[place],
             device(xs(h), 2 * y_hi + r, z, c), False)

        @pl.when(place == row)
        def _():
            owned[row, 0] = ys[2 * i]
            owned[row, 1] = ys[2 * i + 1]

    def await_rhs(h):
        for r in range(2):
            row = 2 * h + r

            @pl.when(place != row)
            def _():
                arrived(rhs.at[row], rhs_sem.at[row])

            @pl.when(place == row)
            def _():
                psi_here.wait()

    def await_y(j):
        arrived(ys.at[pl.ds(2 * j, 2)], y_sem.at[j])

    def by_columns(h, arriving):
        count = 2 * xs(h)

        def step(j, carry):
            pl.when(arriving(j))(lambda: await_y(j))
            update(2 * h, j)
            update(2 * h + 1, j)
            return carry

        lax.fori_loop(0, count, step, 0)
        solve(2 * h, count)
        deliver(h, 0)
        update(2 * h + 1, count)
        solve(2 * h + 1, count + 1)
        deliver(h, 1)

    def by_rows(h):
        count = 2 * xs(h)
        for r in range(2):
            def step(j, carry, r=r):
                update(2 * h + r, j)
                return carry

            lax.fori_loop(0, count + r, step, 0)
            solve(2 * h + r, count + r)
            deliver(h, r)

    with jax.named_scope("line"):
        line(h_own, 1)
        line(h_other, 0)
        line(h_own, 2)
        line(h_other, 1)
        line(h_own, 3)
        line(h_other, 2)
        line(h_other, 3)
    with jax.named_scope("across01"):
        across(0, 1)
        for k in range(4):
            for a in range(2):
                over(1, a, k, 0)
    with jax.named_scope("across02"):
        across(0, 2)
    with jax.named_scope("across03"):
        across(0, 3)
        await_rhs(0)

    with jax.named_scope("early"):
        @pl.when(outer)
        def _():
            by_columns(0, lambda j: j < 0)

    with jax.named_scope("across11"):
        across(1, 1)
    with jax.named_scope("across12"):
        across(1, 2)
        await_rhs(1)

    with jax.named_scope("inner"):
        @pl.when(jnp.logical_not(outer))
        def _():
            by_columns(0, lambda j: j >= 0)

    with jax.named_scope("across13"):
        across(1, 3)
    with jax.named_scope("last"):
        @pl.when(outer)
        def _():
            by_columns(1, lambda j: j >= 2)

        @pl.when(jnp.logical_not(outer))
        def _():
            by_rows(1)

    writes = []
    with jax.named_scope("product"):
        for q in range(4):
            pl.when(place != q)(lambda: arrived(owned.at[q], own_sem.at[q]))
            for a in range(2):
                write = pltpu.make_async_copy(
                    owned.at[q, a], out.at[256 * a : 256 * a + 256, 128 * q : 128 * q + 128],
                    local_sem.at[3 + 2 * q + a],
                )
                write.start()
                writes.append(write)
            block = owned[q].reshape(512, 128)
            term = product(block, block, (((1,), (1,)), ((), ())))
            if q == 0:
                part[...] = term
            else:
                part[...] = part[...] + term

    lines = pl.ds(pl.multiple_of(256 * c, 256), 256)
    other = pl.ds(pl.multiple_of(256 - 256 * c, 256), 256)
    with jax.named_scope("halves"):
        send(None, part.at[other], half, half_sem.at[0], half_sem.at[1], device(x, y, z, 1 - c))
        arrived(half, half_sem.at[1])
        half[...] = half[...] + part[lines, :]
    m = j_own
    with jax.named_scope("scatter"):
        for t in range(1, 8):
            to = lax.rem(m + t, 8)
            send(None, half.at[pl.ds(pl.multiple_of(32 * to, 32), 32)], pieces.at[t - 1],
                 rs_send.at[t - 1], rs_sem.at[t - 1],
                 device(x, 2 * (to % 2) + y_lo, to // 2, c))
        total = half[pl.ds(pl.multiple_of(32 * m, 32), 32), :]
        for t in range(1, 8):
            arrived(pieces.at[t - 1], rs_sem.at[t - 1])
            total = total + pieces[t - 1]
        mine = c * 8 + m
        whole[mine] = total * (1.0 / NG)
    with jax.named_scope("spread"):
        for t in range(1, 8):
            to = lax.rem(m + t, 8)
            send(None, whole.at[mine], whole.at[mine], ag_send.at[t - 1], ag_sem.at[mine],
                 device(x, 2 * (to % 2) + y_lo, to // 2, c))
        send(None, whole.at[mine], whole.at[mine], ag_cross.at[0], ag_sem.at[mine],
             device(x, y, z, 1 - c))
        for t in range(1, 8):
            at = c * 8 + lax.rem(m + 8 - t, 8)
            arrived(whole.at[at], ag_sem.at[at])
            send(None, whole.at[at], whole.at[at], ag_cross.at[t], ag_sem.at[at],
                 device(x, y, z, 1 - c))
        for t in range(8):
            at = (1 - c) * 8 + t
            arrived(whole.at[at], ag_sem.at[at])
    final = pltpu.make_async_copy(whole, inter, local_sem.at[11])
    final.start()
    for cond, copy in pending:
        if cond is None:
            copy.wait_send()
        else:
            pl.when(cond)(copy.wait_send)
    send_later()
    for row in range(4):
        i = 2 * xs(row // 2) + row % 2
        block = ys.at[pl.ds(2 * i, 2)]
        if row < 2:
            arrived(block, y_send.at[row])
        else:
            pl.when(jnp.logical_not(outer))(lambda: arrived(block, y_send.at[row]))
        pl.when(place != row)(lambda: arrived(block, own_send.at[row]))
    for write in writes:
        write.wait()
    final.wait()


def local(psi, lower):
    dma = pltpu.SemaphoreType.DMA
    out, inter = pl.pallas_call(
        kernel,
        out_shape=(
            jax.ShapeDtypeStruct((512, 512), F32),
            jax.ShapeDtypeStruct((16, 32, 512), F32),
        ),
        in_specs=[pl.BlockSpec(memory_space=pl.ANY)] * 2,
        out_specs=(pl.BlockSpec(memory_space=pl.ANY),) * 2,
        scratch_shapes=[
            pltpu.VMEM((128, 256, 256), F32),
            pltpu.VMEM((16, 256, 128), F32),
            pltpu.VMEM((4, 512, 128), F32),
            pltpu.VMEM((4, 2, 256, 128), F32),
            pltpu.VMEM((512, 512), F32),
            pltpu.VMEM((256, 512), F32),
            pltpu.VMEM((7, 32, 512), F32),
            pltpu.VMEM((16, 32, 512), F32),
            pltpu.VMEM((256, 256), F32),
            dma((128,)), dma((12,)), dma((48,)), dma((64,)), dma((2,)), dma((4,)), dma((4,)),
            dma((8,)), dma((4,)), dma((4,)), dma((4,)), dma((2,)), dma((7,)), dma((7,)),
            dma((16,)), dma((7,)), dma((8,)), dma((12,)),
        ],
        compiler_params=pltpu.CompilerParams(
            has_side_effects=True, collective_id=0, vmem_limit_bytes=60 * 1024 * 1024
        ),
    )(psi, lower)
    return out, inter.reshape(512, 512)


def solution(mesh):
    return jax.shard_map(
        local,
        mesh=mesh,
        in_specs=(P("band", "ga"), P("band", "ga")),
        out_specs=(P("band", "ga"), P("band", None)),
        check_vma=False,
    )
```

```python
import jax
import jax.numpy as jnp
from jax import lax
from jax.experimental import pallas as pl
from jax.experimental.pallas import tpu as pltpu
from jax.sharding import PartitionSpec as P

MESH = pl.DeviceIdType.MESH
F32 = jnp.float32
BF16 = jnp.bfloat16
NG = 8192


def split(a):
    high = a.astype(BF16)
    return high, (a - high.astype(F32)).astype(BF16)


def product(a, b, dims=(((1,), (0,)), ((), ()))):
    ah, al = split(a)
    bh, bl = split(b)

    def dot(p, q):
        return lax.dot_general(p, q, dims, preferred_element_type=F32)

    return dot(ah, bh) + (dot(ah, bl) + dot(al, bh))


def kernel(
    psi, lower, out, inter,
    tiles, ys, rhs, owned, part, half, pieces, whole, inverse,
    tile_sem, ring_sem, cross_sem, pair_sem, swap_sem, rhs_sem, rhs_send,
    y_sem, y_send, own_sem, own_send, half_sem, rs_sem, rs_send, ag_sem, ag_send,
    ag_cross, local_sem,
):
    band = lax.axis_index("band")
    ga = lax.axis_index("ga")
    x, y_lo = band // 2, band % 2
    z, y_hi, c = ga // 4, (ga // 2) % 2, ga % 2
    y = 2 * y_hi + y_lo
    h_own = x // 2
    outer = jnp.logical_or(x == 0, x == 3)
    x_low = jnp.minimum(x, 3 - x)
    place = 2 * h_own + y_lo

    def device(dx, dy, dz, dc):
        return (2 * dx + dy % 2, 4 * dz + 2 * (dy // 2) + dc)

    def xs(h):
        return x_low * (1 - h) + (3 - x_low) * h

    def slot(row, j, a, b):
        return ((row * 8 + j) * 2 + a) * 2 + b

    pending = []

    def send(cond, src, dst, s_sem, r_sem, target, later=True):
        copy = pltpu.make_async_remote_copy(
            src_ref=src, dst_ref=dst, send_sem=s_sem, recv_sem=r_sem,
            device_id=target, device_id_type=MESH,
        )
        if cond is None:
            copy.start()
        else:
            pl.when(cond)(copy.start)
        if later:
            pending.append((cond, copy))
        return copy

    def arrived(ref, sem):
        pltpu.make_async_copy(ref, ref, sem).wait()

    j_own = 2 * z + y_hi
    loads = []
    for a in range(2):
        load = pltpu.make_async_copy(
            lower.at[256 * a : 256 * a + 256, :], tiles.at[slot(place, j_own, a, c)],
            local_sem.at[1 + a],
        )
        load.start()
        loads.append(load)
    psi_here = pltpu.make_async_copy(
        psi.at[:, pl.ds(pl.multiple_of(128 * place, 128), 128)], rhs.at[place], local_sem.at[0]
    )
    psi_here.start()

    def place_of(v):
        return lax.rem(v + 8, 4)

    barrier = pltpu.get_barrier_semaphore()
    friends = [
        (3 - x, y, z, c), (x, 2 * y_hi + 1 - y_lo, z, c), (3 - x, 2 * y_hi + 1 - y_lo, z, c),
        (x + 1 - 2 * (x % 2), y, z, c), (x, y, z, 1 - c),
        (x, place_of(y + 1), z, c), (x, place_of(y - 1), z, c),
        (x, y, place_of(z + 1), c), (x, y, place_of(z - 1), c),
    ] + [
        (x, 2 * (lax.rem(j_own + t, 8) % 2) + y_lo, lax.rem(j_own + t, 8) // 2, c)
        for t in range(1, 8)
    ]
    for friend in friends:
        pl.semaphore_signal(barrier, inc=1, device_id=device(*friend), device_id_type=MESH)
    pl.semaphore_wait(barrier, len(friends))
    for load in loads:
        load.wait()

    def quarter(h, a, k, s):
        sgn = 1 - 2 * a
        yo = place_of(y - sgn * (k * c + s * (1 - c)))
        zo = place_of(z - sgn * (k * (1 - c) + s * c))
        row, j = 2 * h + yo % 2, 2 * zo + yo // 2
        i = 2 * xs(h) + yo % 2
        here = slot(row, j, a, c)
        return here, 2 * j + c <= 2 * i + a

    def await_quarter(h, a, k, s):
        here, real = quarter(h, a, k, s)
        pl.when(real)(lambda: arrived(tiles.at[here], tile_sem.at[here]))

    def along(h, a, k, also=None):
        here, real = quarter(h, a, k, 0)
        sgn = 1 - 2 * a
        cond = real if also is None else jnp.logical_and(real, also)
        ref = tiles.at[here]
        send(cond, ref, ref, ring_sem.at[(h * 2 + a) * 3 + k], tile_sem.at[here],
             device(x, place_of(y + sgn * c), place_of(z + sgn * (1 - c)), c))

    def over(h, a, k, s, also=None):
        here, real = quarter(h, a, k, s)
        sgn = 1 - 2 * a
        cond = real if also is None else jnp.logical_and(real, also)
        ref = tiles.at[here]
        send(cond, ref, ref, cross_sem.at[((h * 2 + a) * 4 + k) * 3 + s], tile_sem.at[here],
             device(x, place_of(y + sgn * (1 - c)), place_of(z + sgn * c), c))

    def to_sibling(h, a, k, s, also=None):
        here, real = quarter(h, a, k, s)
        cond = real if also is None else jnp.logical_and(real, also)
        ref = tiles.at[here]
        send(cond, ref, ref, pair_sem.at[((h * 2 + a) * 4 + k) * 4 + s], tile_sem.at[here],
             device(x, y, z, 1 - c))

    h_other = 1 - h_own
    diagonal = j_own == band

    def own_quarters(ready):
        for a in range(2):
            here, real = quarter(h_own, a, 0, 0)
            send(jnp.logical_and(real, ready(a)), tiles.at[here], tiles.at[here],
                 swap_sem.at[a], tile_sem.at[here], device(3 - x, y, z, c), False)
        for a in range(2):
            along(h_own, a, 0, ready(a))
        for a in range(2):
            over(h_own, a, 0, 0, jnp.logical_and(ready(a), h_own == 0))
            to_sibling(h_own, a, 0, 0, ready(a))

    def finish_sends():
        for cond, copy in pending:
            if cond is None:
                copy.wait_send()
            else:
                pl.when(cond)(copy.wait_send)
        pending.clear()

    def send_later():
        for a in range(2):
            here, real = quarter(h_own, a, 0, 0)
            pl.when(real)(lambda: arrived(tiles.at[here], swap_sem.at[a]))

    own_quarters(lambda a: jnp.logical_not(jnp.logical_and(diagonal, c == a)))

    @pl.when(diagonal)
    def _():
        where = slot(place, j_own, c, c)
        rows = lax.broadcasted_iota(jnp.int32, (256, 256), 0)
        cols = lax.broadcasted_iota(jnp.int32, (256, 256), 1)
        tri = tiles[where]
        diag = jnp.where(rows == cols, tri, 0.0)
        down = 1.0 / jnp.sum(diag, axis=1, keepdims=True)
        across = 1.0 / jnp.sum(diag, axis=0, keepdims=True)
        pairs = jnp.logical_and(rows == cols + 1, rows % 2 == 1)
        inverse[...] = jnp.where(rows == cols, down, 0.0) - jnp.where(
            pairs, tri * down * across, 0.0
        )

        def level(k, carry):
            rk, ck = rows >> k, cols >> k
            inside = jnp.logical_and(rk == ck + 1, rk % 2 == 1)
            below = jnp.where(inside, tiles[where], 0.0)
            now = inverse[...]
            inverse[...] = now - product(now, product(below, now))
            return carry

        lax.fori_loop(1, 8, level, 0)
        tiles[where] = inverse[...]

    own_quarters(lambda a: jnp.logical_and(diagonal, c == a))

    def share_rhs(when):
        for q in range(4):
            send(
                jnp.logical_and(place != q, when),
                psi.at[:, 128 * q : 128 * q + 128], rhs.at[place],
                rhs_send.at[q], rhs_sem.at[place],
                device(xs(q // 2), 2 * y_hi + q % 2, z, c),
            )

    def line(h, k):
        for a in range(2):
            await_quarter(h, a, k, 0)
            if k < 3:
                along(h, a, k)
            over(h, a, k, 0, h == 0)
            to_sibling(h, a, k, 0)

    def across(h, s):
        for k in range(4):
            for a in range(2):
                await_quarter(h, a, k, s)
                if s < 3:
                    over(h, a, k, s)
                to_sibling(h, a, k, s)

    def tile(row, j, a, b):
        return tiles[slot(row, j, a, b)]

    def from_sibling(row, j, a):
        here = slot(row, j, a, 1 - c)
        arrived(tiles.at[here], tile_sem.at[here])

    def update(row, j):
        for a in range(2):
            from_sibling(row, j, a)
        top, bottom = ys[2 * j], ys[2 * j + 1]
        for a in range(2):
            rhs[row, 256 * a : 256 * a + 256, :] = rhs[row, 256 * a : 256 * a + 256, :] - (
                product(tile(row, j, a, 0), top) + product(tile(row, j, a, 1), bottom)
            )

    def deliver(h, r, part_no):
        row = 2 * h + r
        i = 2 * xs(h) + r
        block = ys.at[2 * i + part_no]
        send(None if h == 0 else jnp.logical_not(outer), block, block,
             y_send.at[2 * row + part_no], y_sem.at[2 * i + part_no],
             device(x + 1 - 2 * (x % 2), y, z, c), False)
        send(place != row, block, owned.at[place, part_no], own_send.at[2 * row + part_no],
             own_sem.at[place, part_no], device(xs(h), 2 * y_hi + r, z, c), False)

        @pl.when(place == row)
        def _():
            owned[row, part_no] = ys[2 * i + part_no]

    def solve(h, r):
        row = 2 * h + r
        i = 2 * xs(h) + r

        @pl.when(c == 0)
        def _():
            from_sibling(row, i, 1)

        @pl.when(c == 1)
        def _():
            from_sibling(row, i, 0)
            from_sibling(row, i, 1)

        top = product(tile(row, i, 0, 0), rhs[row, 0:256, :])
        ys[2 * i] = top
        deliver(h, r, 0)
        bottom = product(
            tile(row, i, 1, 1), rhs[row, 256:512, :] - product(tile(row, i, 1, 0), top)
        )
        ys[2 * i + 1] = bottom
        deliver(h, r, 1)

    def await_rhs(h):
        for r in range(2):
            row = 2 * h + r

            @pl.when(place != row)
            def _():
                arrived(rhs.at[row], rhs_sem.at[row])

            @pl.when(place == row)
            def _():
                psi_here.wait()

    def await_y(j):
        for part_no in range(2):
            arrived(ys.at[2 * j + part_no], y_sem.at[2 * j + part_no])

    def by_columns(h, arriving):
        count = 2 * xs(h)

        def step(j, carry):
            pl.when(arriving(j))(lambda: await_y(j))
            update(2 * h, j)
            update(2 * h + 1, j)
            return carry

        lax.fori_loop(0, count, step, 0)
        solve(h, 0)
        update(2 * h + 1, count)
        solve(h, 1)

    def by_rows(h):
        count = 2 * xs(h)
        for r in range(2):
            def step(j, carry, r=r):
                update(2 * h + r, j)
                return carry

            lax.fori_loop(0, count + r, step, 0)
            solve(h, r)

    def begin_over(h):
        for k in range(4):
            for a in range(2):
                over(h, a, k, 0)

    share_rhs(h_own == 0)
    with jax.named_scope("line"):
        line(h_other, 0)
        line(0, 1)
        line(1, 1)
        line(0, 2)
        line(0, 3)
    with jax.named_scope("across01"):
        across(0, 1)
        line(1, 2)
    with jax.named_scope("across02"):
        across(0, 2)
        line(1, 3)
        begin_over(1)
        share_rhs(h_own == 1)
    with jax.named_scope("across03"):
        across(0, 3)
        await_rhs(0)

    with jax.named_scope("early"):
        @pl.when(outer)
        def _():
            by_columns(0, lambda j: j < 0)

    with jax.named_scope("across11"):
        across(1, 1)
    with jax.named_scope("across12"):
        across(1, 2)
        await_rhs(1)

    with jax.named_scope("inner"):
        @pl.when(jnp.logical_not(outer))
        def _():
            by_columns(0, lambda j: j >= 0)

    with jax.named_scope("across13"):
        across(1, 3)
    with jax.named_scope("last"):
        @pl.when(outer)
        def _():
            by_columns(1, lambda j: j >= 2)

        @pl.when(jnp.logical_not(outer))
        def _():
            by_rows(1)

    with jax.named_scope("settle"):
        finish_sends()
        send_later()
        for row in range(4):
            for part_no in range(2):
                block = ys.at[2 * (2 * xs(row // 2) + row % 2) + part_no]
                sem = y_send.at[2 * row + part_no]
                if row < 2:
                    arrived(block, sem)
                else:
                    pl.when(jnp.logical_not(outer))(lambda: arrived(block, sem))
                pl.when(place != row)(lambda: arrived(block, own_send.at[2 * row + part_no]))

    writes = []
    with jax.named_scope("product"):
        beside = place + 1 - 2 * (place % 2)
        for n, q in enumerate(
            (place, beside, lax.rem(place + 2, 4), lax.rem(beside + 2, 4))
        ):
            for a in range(2):
                if n:
                    arrived(owned.at[q, a], own_sem.at[q, a])
                write = pltpu.make_async_copy(
                    owned.at[q, a],
                    out.at[
                        256 * a : 256 * a + 256, pl.ds(pl.multiple_of(128 * q, 128), 128)
                    ],
                    local_sem.at[3 + 2 * n + a],
                )
                write.start()
                writes.append(write)
            block = owned[q].reshape(512, 128)
            at = 0
            for r in range(4):
                term = product(
                    block[128 * r : 128 * r + 128], block[: 128 * r + 128],
                    (((1,), (1,)), ((), ())),
                )
                for s in range(r + 1):
                    here = term[:, 128 * s : 128 * s + 128]
                    part[at] = here if n == 0 else part[at] + here
                    at += 1

    with jax.named_scope("halves"):
        send(None, part.at[pl.ds(5 - 5 * c, 5)], half, half_sem.at[0], half_sem.at[1],
             device(x, y, z, 1 - c))
        arrived(half, half_sem.at[1])
        half[...] = half[...] + part[pl.ds(5 * c, 5)]
    m = j_own

    def lines(of):
        return pl.ds(pl.multiple_of(16 * of, 16), 16)

    with jax.named_scope("scatter"):
        for t in range(1, 8):
            to = lax.rem(m + t, 8)
            send(None, half.at[:, lines(to)], pieces.at[t - 1],
                 rs_send.at[t - 1], rs_sem.at[t - 1],
                 device(x, 2 * (to % 2) + y_lo, to // 2, c))
        total = half[:, lines(m), :]
        for t in range(1, 8):
            arrived(pieces.at[t - 1], rs_sem.at[t - 1])
            total = total + pieces[t - 1]
        whole[c, :, lines(m), :] = total * (1.0 / NG)
    with jax.named_scope("spread"):
        def share(core, of, s_sem, target):
            ref = whole.at[core, :, lines(of)]
            send(None, ref, ref, s_sem, ag_sem.at[core * 8 + of], target)

        for t in range(1, 8):
            to = lax.rem(m + t, 8)
            share(c, m, ag_send.at[t - 1], device(x, 2 * (to % 2) + y_lo, to // 2, c))
        share(c, m, ag_cross.at[0], device(x, y, z, 1 - c))
        for t in range(1, 8):
            of = lax.rem(m + 8 - t, 8)
            arrived(whole.at[c, :, lines(of)], ag_sem.at[c * 8 + of])
            share(c, of, ag_cross.at[t], device(x, y, z, 1 - c))
        for of in range(8):
            arrived(whole.at[1 - c, :, lines(of)], ag_sem.at[(1 - c) * 8 + of])
        at = 0
        for r in range(4):
            for s in range(r + 1):
                block = whole[at // 5, at % 5]
                inter[128 * r : 128 * r + 128, 128 * s : 128 * s + 128] = block
                if s < r:
                    inter[128 * s : 128 * s + 128, 128 * r : 128 * r + 128] = block.T
                at += 1
    finish_sends()
    for write in writes:
        write.wait()


def local(psi, lower):
    dma = pltpu.SemaphoreType.DMA
    out, inter = pl.pallas_call(
        kernel,
        out_shape=(
            pltpu.VMEM((512, 512), F32),
            pltpu.VMEM((512, 512), F32),
        ),
        in_specs=[pl.BlockSpec(memory_space=pl.ANY)] * 2,
        out_specs=(pl.BlockSpec(memory_space=pltpu.VMEM),) * 2,
        scratch_shapes=[
            pltpu.VMEM((128, 256, 256), F32),
            pltpu.VMEM((16, 256, 128), F32),
            pltpu.VMEM((4, 512, 128), F32),
            pltpu.VMEM((4, 2, 256, 128), F32),
            pltpu.VMEM((10, 128, 128), F32),
            pltpu.VMEM((5, 128, 128), F32),
            pltpu.VMEM((7, 5, 16, 128), F32),
            pltpu.VMEM((2, 5, 128, 128), F32),
            pltpu.VMEM((256, 256), F32),
            dma((128,)), dma((12,)), dma((48,)), dma((64,)), dma((2,)), dma((4,)), dma((4,)),
            dma((16,)), dma((8,)), dma((4, 2)), dma((8,)), dma((2,)), dma((7,)), dma((7,)),
            dma((16,)), dma((7,)), dma((8,)), dma((12,)),
        ],
        compiler_params=pltpu.CompilerParams(
            has_side_effects=True, collective_id=0, vmem_limit_bytes=60 * 1024 * 1024
        ),
    )(psi, lower)
    return out, inter


def solution(mesh):
    return jax.shard_map(
        local,
        mesh=mesh,
        in_specs=(P("band", "ga"), P("band", "ga")),
        out_specs=(P("band", "ga"), P("band", None)),
        check_vma=False,
    )
```

```python
import jax
import jax.numpy as jnp
from jax import lax
from jax.experimental import pallas as pl
from jax.experimental.pallas import tpu as pltpu
from jax.sharding import PartitionSpec as P

MESH = pl.DeviceIdType.MESH
F32 = jnp.float32
BF16 = jnp.bfloat16
NG = 8192

EVENTS = (
    (405115079, 138699458, 461177167, 540649354, 326504717, 695371218, 357657612,
     602061930, 867409058, 882306733, 1037815163, 1054767524, 4079),
    (421552280, 154706183, 51775376, 525972442, 295774283, 695256916, 390912688,
     952720171, 986896625, 668702899, 905070958, 1037987771, 4079),
    (537428547, 86553697, 676088400, 339051673, 113447715, 128820586, 266742939,
     476001720, 764594510, 899395293, 800714023, 937152351, 4094),
    (170143880, 276869381, 122324065, 322081165, 408049898, 246216880, 616932697,
     850754028, 870431126, 884709167, 519023965, 1054830367, 4093),
    (9079395, 723717185, 949397769, 300360755, 655282818, 422414764, 988619076,
     213599477, 102553263, 937150164, 477422973, 402646415, 2014),
    (697182720, 613714561, 180556139, 43696324, 868932041, 959639056, 114340335,
     1005134965, 926377492, 256886350, 486106813, 492692827, 4063),
    (419860520, 52791459, 264574160, 734032607, 605664712, 313058149, 98936670,
     751313592, 72963852, 871029140, 936856507, 1073471271, 3062),
    (580917824, 588808450, 705459150, 177333925, 414043185, 455393631, 429554443,
     347432080, 944193117, 844946351, 1005280531, 1039228406, 4094),
)
SHARE_AT = (19, 23, 22, 23, 22, 23, 22, 26)
STAGE_AT = (35, 42, 59, 59, 62, 62, 49, 59)
EVENT_COUNT = (62, 62, 62, 62, 62, 62, 62, 62)


def split(a):
    high = a.astype(BF16)
    return high, (a - high.astype(F32)).astype(BF16)


def product(a, b, dims=(((1,), (0,)), ((), ()))):
    ah, al = split(a)
    bh, bl = split(b)

    def dot(p, q):
        return lax.dot_general(p, q, dims, preferred_element_type=F32)

    return dot(ah, bh) + (dot(ah, bl) + dot(al, bh))


def narrow_product(a, b):
    ah, al = split(a)
    bh, bl = split(b)
    wide = jnp.dot(ah, jnp.concatenate([bh, bl], axis=1), preferred_element_type=F32)
    rest = jnp.dot(al, bh, preferred_element_type=F32)
    return wide[:, :128] + (wide[:, 128:] + rest)


def kernel(
    psi, lower, out, inter,
    tiles, ys, rhs, owned, part, half, pieces, whole, inverse,
    tile_sem, ring_sem, back_sem, cross_sem, return_sem, pair_sem, swap_sem, rhs_sem, rhs_send,
    y_sem, y_send, own_sem, own_send, half_sem, rs_sem, rs_send, ag_sem, ag_send,
    ag_cross, local_sem,
):
    band = lax.axis_index("band")
    ga = lax.axis_index("ga")
    x, y_lo = band // 2, band % 2
    z, y_hi, c = ga // 4, (ga // 2) % 2, ga % 2
    y = 2 * y_hi + y_lo
    h_own = x // 2
    outer = jnp.logical_or(x == 0, x == 3)
    x_low = jnp.minimum(x, 3 - x)
    place = 2 * h_own + y_lo

    def device(dx, dy, dz, dc):
        return (2 * dx + dy % 2, 4 * dz + 2 * (dy // 2) + dc)

    def xs(h):
        return x_low * (1 - h) + (3 - x_low) * h

    def slot(row, j, a, b):
        return ((row * 8 + j) * 2 + a) * 2 + b

    pending = []

    def send(cond, src, dst, s_sem, r_sem, target, later=True):
        copy = pltpu.make_async_remote_copy(
            src_ref=src, dst_ref=dst, send_sem=s_sem, recv_sem=r_sem,
            device_id=target, device_id_type=MESH,
        )
        if cond is None:
            copy.start()
        else:
            pl.when(cond)(copy.start)
        if later:
            pending.append((cond, copy))
        return copy

    def arrived(ref, sem):
        pltpu.make_async_copy(ref, ref, sem).wait()

    j_own = 2 * z + y_hi
    loads = []
    for a in range(2):
        load = pltpu.make_async_copy(
            lower.at[256 * a : 256 * a + 256, :], tiles.at[slot(place, j_own, a, c)],
            local_sem.at[1 + a],
        )
        load.start()
        loads.append(load)
    psi_here = pltpu.make_async_copy(
        psi.at[:, pl.ds(pl.multiple_of(128 * place, 128), 128)], rhs.at[place], local_sem.at[0]
    )
    psi_here.start()

    def place_of(v):
        return lax.rem(v + 8, 4)

    barrier = pltpu.get_barrier_semaphore()
    friends = [
        (3 - x, y, z, c), (x, 2 * y_hi + 1 - y_lo, z, c), (3 - x, 2 * y_hi + 1 - y_lo, z, c),
        (x + 1 - 2 * (x % 2), y, z, c), (x, y, z, 1 - c),
        (x, place_of(y + 1), z, c), (x, place_of(y - 1), z, c),
        (x, y, place_of(z + 1), c), (x, y, place_of(z - 1), c),
    ] + [
        (x, 2 * (lax.rem(j_own + t, 8) % 2) + y_lo, lax.rem(j_own + t, 8) // 2, c)
        for t in range(1, 8)
    ]
    for friend in friends:
        pl.semaphore_signal(barrier, inc=1, device_id=device(*friend), device_id_type=MESH)
    pl.semaphore_wait(barrier, len(friends))
    for load in loads:
        load.wait()

    def quarter(h, a, k, s):
        sgn = 1 - 2 * a
        yo = place_of(y - sgn * (k * c + s * (1 - c)))
        zo = place_of(z - sgn * (k * (1 - c) + s * c))
        row, j = 2 * h + yo % 2, 2 * zo + yo // 2
        i = 2 * xs(h) + yo % 2
        here = slot(row, j, a, c)
        return here, 2 * j + c <= 2 * i + a

    diagonal = j_own == band

    def both(*conds):
        out = conds[0]
        for cond in conds[1:]:
            out = jnp.logical_and(out, cond)
        return out

    def by_pair(h, k, s):
        far = jnp.logical_or(k > 0, s > 0)
        return jnp.logical_or(
            both(outer, h == 0, far),
            both(k == 0, s > 0, jnp.logical_or(h == 1, jnp.logical_not(outer))),
        )

    def copies(h, a, k, s):
        here, real = quarter(h, a, k, s)
        sgn = 1 - 2 * a
        ours = h == h_own
        short1 = short2 = both(outer, h == 0)
        ref = tiles.at[here]

        def along(m):
            return device(x, place_of(y + m * c), place_of(z + m * (1 - c)), c)

        def over(m):
            return device(x, place_of(y + m * (1 - c)), place_of(z + m * c), c)

        def ring(k2, s2):
            return both(real, jnp.logical_or(ours, jnp.logical_not(by_pair(h, k2, s2))))

        last1 = 3 - short1.astype(jnp.int32)
        last2 = 3 - short2.astype(jnp.int32)
        near = both(k == 0, s == 0)
        line = (h * 4 + k) * 2 + a
        for cond, sem, target in (
            (both(real, ours, jnp.logical_or(near, by_pair(h, k, s))),
             swap_sem.at[line * 4 + s], device(3 - x, y, z, c)),
            (both(ring(k + 1, 0), s == 0, k < last1),
             ring_sem.at[line], along(sgn)),
            (both(ring(3, 0), near, short1), back_sem.at[h * 2 + a], along(-sgn)),
            (both(ring(k, s + 1), s < last2), cross_sem.at[line * 4 + s], over(sgn)),
            (both(ring(k, 3), s == 0, short2), return_sem.at[line], over(-sgn)),
            (real, pair_sem.at[line * 4 + s], device(x, y, z, 1 - c)),
        ):
            yield cond, pltpu.make_async_remote_copy(
                src_ref=ref, dst_ref=ref, send_sem=sem, recv_sem=tile_sem.at[here],
                device_id=target, device_id_type=MESH,
            )

    def finish_sends():
        for cond, copy in pending:
            if cond is None:
                copy.wait_send()
            else:
                pl.when(cond)(copy.wait_send)
        pending.clear()

    def own_quarters(ready):
        for a in range(2):
            for cond, copy in copies(h_own, a, 0, 0):
                pl.when(both(cond, ready(a)))(copy.start)

    def decode(code):
        return code // 32, code % 2, (code // 8) % 4, (code // 2) % 4

    kind = 2 * x + c

    def by_kind(values):
        out = jnp.int32(values[0])
        for n, value in enumerate(values[1:]):
            out = jnp.where(kind == n + 1, jnp.int32(value), out)
        return out

    words = [by_kind(word) for word in zip(*EVENTS)]

    def event(n, carry):
        which = n // 5
        word = words[0]
        for at, other in enumerate(words[1:]):
            word = jnp.where(which == at + 1, other, word)
        h, a, k, s = decode(lax.shift_right_logical(word, 6 * (n % 5)) % 64)
        here, real = quarter(h, a, k, s)
        pl.when(both(real, jnp.logical_not(both(h == h_own, k == 0, s == 0))))(
            lambda: arrived(tiles.at[here], tile_sem.at[here])
        )
        for cond, copy in copies(h, a, k, s):
            pl.when(cond)(copy.start)
        return carry

    def sent(code, carry):
        for cond, copy in copies(*decode(code)):
            pl.when(cond)(copy.wait_send)
        return carry

    own_quarters(lambda a: jnp.logical_not(both(diagonal, c == a)))

    @pl.when(diagonal)
    def _():
        where = slot(place, j_own, c, c)
        rows = lax.broadcasted_iota(jnp.int32, (256, 256), 0)
        cols = lax.broadcasted_iota(jnp.int32, (256, 256), 1)
        tri = tiles[where]
        diag = jnp.where(rows == cols, tri, 0.0)
        down = 1.0 / jnp.sum(diag, axis=1, keepdims=True)
        across = 1.0 / jnp.sum(diag, axis=0, keepdims=True)
        pairs = jnp.logical_and(rows == cols + 1, rows % 2 == 1)
        inverse[...] = jnp.where(rows == cols, down, 0.0) - jnp.where(
            pairs, tri * down * across, 0.0
        )

        def level(k, carry):
            rk, ck = rows >> k, cols >> k
            inside = jnp.logical_and(rk == ck + 1, rk % 2 == 1)
            below = jnp.where(inside, tiles[where], 0.0)
            now = inverse[...]
            inverse[...] = now - product(now, product(below, now))
            return carry

        lax.fori_loop(1, 8, level, 0)
        tiles[where] = inverse[...]

    own_quarters(lambda a: both(diagonal, c == a))

    def share_rhs(when):
        for q in range(4):
            send(
                jnp.logical_and(place != q, when),
                psi.at[:, 128 * q : 128 * q + 128], rhs.at[place],
                rhs_send.at[q], rhs_sem.at[place],
                device(xs(q // 2), 2 * y_hi + q % 2, z, c),
            )

    def tile(row, j, a, b):
        return tiles[slot(row, j, a, b)]

    def from_sibling(row, j, a):
        here = slot(row, j, a, 1 - c)
        arrived(tiles.at[here], tile_sem.at[here])

    def update(row, j):
        for a in range(2):
            from_sibling(row, j, a)
        top, bottom = ys[2 * j], ys[2 * j + 1]
        for a in range(2):
            rhs[row, 256 * a : 256 * a + 256, :] = rhs[row, 256 * a : 256 * a + 256, :] - (
                narrow_product(tile(row, j, a, 0), top) + narrow_product(tile(row, j, a, 1), bottom)
            )

    def deliver(h, r, part_no):
        row = 2 * h + r
        i = 2 * xs(h) + r
        block = ys.at[2 * i + part_no]
        send(None if h == 0 else jnp.logical_not(outer), block, block,
             y_send.at[2 * row + part_no], y_sem.at[2 * i + part_no],
             device(x + 1 - 2 * (x % 2), y, z, c), False)
        send(place != row, block, owned.at[place, part_no], own_send.at[2 * row + part_no],
             own_sem.at[place, part_no], device(xs(h), 2 * y_hi + r, z, c), False)

        @pl.when(place == row)
        def _():
            owned[row, part_no] = ys[2 * i + part_no]

    def solve(h, r):
        row = 2 * h + r
        i = 2 * xs(h) + r

        @pl.when(c == 0)
        def _():
            from_sibling(row, i, 1)

        @pl.when(c == 1)
        def _():
            from_sibling(row, i, 0)
            from_sibling(row, i, 1)

        top = narrow_product(tile(row, i, 0, 0), rhs[row, 0:256, :])
        ys[2 * i] = top
        deliver(h, r, 0)
        bottom = narrow_product(
            tile(row, i, 1, 1), rhs[row, 256:512, :] - narrow_product(tile(row, i, 1, 0), top)
        )
        ys[2 * i + 1] = bottom
        deliver(h, r, 1)

    def await_rhs(h):
        for r in range(2):
            row = 2 * h + r

            @pl.when(place != row)
            def _():
                arrived(rhs.at[row], rhs_sem.at[row])

            @pl.when(place == row)
            def _():
                psi_here.wait()

    def await_y(j):
        for part_no in range(2):
            arrived(ys.at[2 * j + part_no], y_sem.at[2 * j + part_no])

    def by_columns(h, arriving):
        count = 2 * xs(h)

        def step(j, carry):
            pl.when(arriving(j))(lambda: await_y(j))
            update(2 * h, j)
            update(2 * h + 1, j)
            return carry

        lax.fori_loop(0, count, step, 0)
        solve(h, 0)
        update(2 * h + 1, count)
        solve(h, 1)

    def by_rows(h):
        count = 2 * xs(h)
        for r in range(2):
            def step(j, carry, r=r):
                update(2 * h + r, j)
                return carry

            lax.fori_loop(0, count + r, step, 0)
            solve(h, r)

    share_at, stage_at, count = by_kind(SHARE_AT), by_kind(STAGE_AT), by_kind(EVENT_COUNT)
    share_rhs(h_own == 0)
    with jax.named_scope("first"):
        lax.fori_loop(0, share_at, event, 0)
    share_rhs(h_own == 1)
    with jax.named_scope("second"):
        lax.fori_loop(share_at, stage_at, event, 0)
    with jax.named_scope("early"):
        await_rhs(0)
        by_columns(0, lambda j: jnp.logical_not(outer))
    with jax.named_scope("third"):
        lax.fori_loop(stage_at, count, event, 0)
    with jax.named_scope("last"):
        await_rhs(1)

        @pl.when(outer)
        def _():
            by_columns(1, lambda j: j >= 2)

        @pl.when(jnp.logical_not(outer))
        def _():
            by_rows(1)

    with jax.named_scope("settle"):
        lax.fori_loop(0, 64, sent, 0)
        finish_sends()
        for row in range(4):
            for part_no in range(2):
                block = ys.at[2 * (2 * xs(row // 2) + row % 2) + part_no]
                sem = y_send.at[2 * row + part_no]
                if row < 2:
                    arrived(block, sem)
                else:
                    pl.when(jnp.logical_not(outer))(lambda: arrived(block, sem))
                pl.when(place != row)(lambda: arrived(block, own_send.at[2 * row + part_no]))

    writes = []
    with jax.named_scope("product"):
        beside = place + 1 - 2 * (place % 2)
        for n, q in enumerate(
            (place, beside, lax.rem(place + 2, 4), lax.rem(beside + 2, 4))
        ):
            for a in range(2):
                if n:
                    arrived(owned.at[q, a], own_sem.at[q, a])
                write = pltpu.make_async_copy(
                    owned.at[q, a],
                    out.at[
                        256 * a : 256 * a + 256, pl.ds(pl.multiple_of(128 * q, 128), 128)
                    ],
                    local_sem.at[3 + 2 * n + a],
                )
                write.start()
                writes.append(write)
            block = owned[q].reshape(512, 128)
            at = 0
            for r in range(4):
                term = product(
                    block[128 * r : 128 * r + 128], block[: 128 * r + 128],
                    (((1,), (1,)), ((), ())),
                )
                for s in range(r + 1):
                    here = term[:, 128 * s : 128 * s + 128]
                    part[at] = here if n == 0 else part[at] + here
                    at += 1

    with jax.named_scope("halves"):
        send(None, part.at[pl.ds(5 - 5 * c, 5)], half, half_sem.at[0], half_sem.at[1],
             device(x, y, z, 1 - c))
        arrived(half, half_sem.at[1])
        half[...] = half[...] + part[pl.ds(5 * c, 5)]
    m = j_own

    def lines(of):
        return pl.ds(pl.multiple_of(16 * of, 16), 16)

    with jax.named_scope("scatter"):
        for t in range(1, 8):
            to = lax.rem(m + t, 8)
            send(None, half.at[:, lines(to)], pieces.at[t - 1],
                 rs_send.at[t - 1], rs_sem.at[t - 1],
                 device(x, 2 * (to % 2) + y_lo, to // 2, c))
        total = half[:, lines(m), :]
        for t in range(1, 8):
            arrived(pieces.at[t - 1], rs_sem.at[t - 1])
            total = total + pieces[t - 1]
        whole[c, :, lines(m), :] = total * (1.0 / NG)
    with jax.named_scope("spread"):
        def share(core, of, s_sem, target):
            ref = whole.at[core, :, lines(of)]
            send(None, ref, ref, s_sem, ag_sem.at[core * 8 + of], target)

        for t in range(1, 8):
            to = lax.rem(m + t, 8)
            share(c, m, ag_send.at[t - 1], device(x, 2 * (to % 2) + y_lo, to // 2, c))
        share(c, m, ag_cross.at[0], device(x, y, z, 1 - c))
        for t in range(1, 8):
            of = lax.rem(m + 8 - t, 8)
            arrived(whole.at[c, :, lines(of)], ag_sem.at[c * 8 + of])
            share(c, of, ag_cross.at[t], device(x, y, z, 1 - c))
        for of in range(8):
            arrived(whole.at[1 - c, :, lines(of)], ag_sem.at[(1 - c) * 8 + of])
        at = 0
        for r in range(4):
            for s in range(r + 1):
                block = whole[at // 5, at % 5]
                inter[128 * r : 128 * r + 128, 128 * s : 128 * s + 128] = block
                if s < r:
                    inter[128 * s : 128 * s + 128, 128 * r : 128 * r + 128] = block.T
                at += 1
    finish_sends()
    for write in writes:
        write.wait()


def local(psi, lower):
    dma = pltpu.SemaphoreType.DMA
    out, inter = pl.pallas_call(
        kernel,
        out_shape=(
            pltpu.VMEM((512, 512), F32),
            pltpu.VMEM((512, 512), F32),
        ),
        in_specs=[pl.BlockSpec(memory_space=pl.ANY)] * 2,
        out_specs=(pl.BlockSpec(memory_space=pltpu.VMEM),) * 2,
        scratch_shapes=[
            pltpu.VMEM((128, 256, 256), F32),
            pltpu.VMEM((16, 256, 128), F32),
            pltpu.VMEM((4, 512, 128), F32),
            pltpu.VMEM((4, 2, 256, 128), F32),
            pltpu.VMEM((10, 128, 128), F32),
            pltpu.VMEM((5, 128, 128), F32),
            pltpu.VMEM((7, 5, 16, 128), F32),
            pltpu.VMEM((2, 5, 128, 128), F32),
            pltpu.VMEM((256, 256), F32),
            dma((128,)), dma((16,)), dma((4,)), dma((64,)), dma((16,)), dma((64,)), dma((64,)),
            dma((4,)), dma((4,)),
            dma((16,)), dma((8,)), dma((4, 2)), dma((8,)), dma((2,)), dma((7,)), dma((7,)),
            dma((16,)), dma((7,)), dma((8,)), dma((12,)),
        ],
        compiler_params=pltpu.CompilerParams(
            has_side_effects=True, collective_id=0, vmem_limit_bytes=60 * 1024 * 1024
        ),
    )(psi, lower)
    return out, inter


def solution(mesh):
    return jax.shard_map(
        local,
        mesh=mesh,
        in_specs=(P("band", "ga"), P("band", "ga")),
        out_specs=(P("band", "ga"), P("band", None)),
        check_vma=False,
    )
```

```python
import jax
import jax.numpy as jnp
from jax import lax
from jax.experimental import pallas as pl
from jax.experimental.pallas import tpu as pltpu
from jax.sharding import PartitionSpec as P

MESH = pl.DeviceIdType.MESH
F32 = jnp.float32
BF16 = jnp.bfloat16
NG = 8192

EVENTS = (
    (136679875, 88367256, 388871135, 239969290, 544596804, 676684961, 348295964,
     952036017, 849057963, 600800054, 1073458023, 613899579, 3964),
    (237002904, 67925577, 437642250, 310163151, 558155168, 950093660, 702887373,
     368028336, 848214818, 783801468, 617605492, 668401087, 3558),
    (538452489, 256250307, 388804112, 963021390, 71926099, 590549846, 998967994,
     527086869, 754079643, 762521917, 666625907, 802581823, 3574),
    (537667080, 68556361, 102545034, 642103824, 204874921, 495905436, 816641255,
     511646692, 364008718, 937921398, 1053387991, 886570746, 3964),
    (10717347, 815241793, 837460516, 281784939, 105193683, 858419335, 1039297388,
     258269912, 391209332, 1069278532, 439547893, 477061982, 1911),
    (696945024, 404912321, 615448942, 801390826, 438933826, 129159561, 283077874,
     457821816, 205861597, 519961909, 233631674, 390055189, 1469),
    (136679425, 454987992, 643703528, 245146579, 275324003, 102171485, 71915458,
     954517270, 714271723, 870140254, 770440626, 886565691, 3964),
    (135798848, 52207886, 596347397, 417641434, 155818331, 278046121, 997576332,
     729368529, 643724144, 1039219820, 365882541, 903020542, 3574),
)
SHARE_AT = (12, 14, 33, 34, 37, 37, 17, 19)
STAGE_AT = (38, 43, 55, 56, 62, 62, 51, 58)
EVENT_COUNT = (62, 62, 62, 62, 62, 62, 62, 62)
BY_PAIR = (49678, 526, 32510, 14)
BOTH_WAYS = (2, 1, 3, 2)


def split(a):
    high = a.astype(BF16)
    return high, (a - high.astype(F32)).astype(BF16)


def product(a, b, dims=(((1,), (0,)), ((), ()))):
    ah, al = split(a)
    bh, bl = split(b)

    def dot(p, q):
        return lax.dot_general(p, q, dims, preferred_element_type=F32)

    return dot(ah, bh) + (dot(ah, bl) + dot(al, bh))


def narrow_product(a, b):
    ah, al = split(a)
    bh, bl = split(b)
    wide = jnp.dot(ah, jnp.concatenate([bh, bl], axis=1), preferred_element_type=F32)
    rest = jnp.dot(al, bh, preferred_element_type=F32)
    return wide[:, :128] + (wide[:, 128:] + rest)


def kernel(
    psi, lower, out, inter,
    tiles, ys, rhs, owned, part, half, pieces, whole, inverse,
    tile_sem, quarter_send, rhs_sem, rhs_send,
    y_sem, y_send, own_sem, own_send, half_sem, rs_sem, rs_send, ag_sem, ag_send,
    ag_cross, local_sem,
):
    band = lax.axis_index("band")
    ga = lax.axis_index("ga")
    x, y_lo = band // 2, band % 2
    z, y_hi, c = ga // 4, (ga // 2) % 2, ga % 2
    y = 2 * y_hi + y_lo
    h_own = x // 2
    outer = jnp.logical_or(x == 0, x == 3)
    x_low = jnp.minimum(x, 3 - x)
    place = 2 * h_own + y_lo

    def device(dx, dy, dz, dc):
        return (2 * dx + dy % 2, 4 * dz + 2 * (dy // 2) + dc)

    def xs(h):
        return x_low * (1 - h) + (3 - x_low) * h

    low, high = 2 * x_low, 2 * (3 - x_low)

    def slot(row, j, a, b):
        before = jnp.where(row > 0, low + 1, 0) + jnp.where(row > 1, low + 2, 0)
        before = before + jnp.where(row > 2, high + 1, 0)
        return ((before + j) * 2 + a) * 2 + b

    pending = []

    def send(cond, src, dst, s_sem, r_sem, target, later=True):
        copy = pltpu.make_async_remote_copy(
            src_ref=src, dst_ref=dst, send_sem=s_sem, recv_sem=r_sem,
            device_id=target, device_id_type=MESH,
        )
        if cond is None:
            copy.start()
        else:
            pl.when(cond)(copy.start)
        if later:
            pending.append((cond, copy))
        return copy

    def arrived(ref, sem):
        pltpu.make_async_copy(ref, ref, sem).wait()

    j_own = 2 * z + y_hi
    loads = []
    for a in range(2):
        load = pltpu.make_async_copy(
            lower.at[256 * a : 256 * a + 256, :], tiles.at[slot(place, j_own, a, c)],
            local_sem.at[1 + a],
        )
        needed = 2 * j_own + c <= 2 * band + a
        pl.when(needed)(load.start)
        loads.append((needed, load))
    psi_here = pltpu.make_async_copy(
        psi.at[:, pl.ds(pl.multiple_of(128 * place, 128), 128)], rhs.at[place], local_sem.at[0]
    )
    psi_here.start()

    def place_of(v):
        return lax.rem(v + 8, 4)

    barrier = pltpu.get_barrier_semaphore()
    friends = [
        (3 - x, y, z, c), (x, 2 * y_hi + 1 - y_lo, z, c), (3 - x, 2 * y_hi + 1 - y_lo, z, c),
        (x + 1 - 2 * (x % 2), y, z, c), (x, y, z, 1 - c),
        (x, place_of(y + 1), z, c), (x, place_of(y - 1), z, c),
        (x, y, place_of(z + 1), c), (x, y, place_of(z - 1), c),
    ] + [
        (x, 2 * (lax.rem(j_own + t, 8) % 2) + y_lo, lax.rem(j_own + t, 8) // 2, c)
        for t in range(1, 8)
    ]
    for friend in friends:
        pl.semaphore_signal(barrier, inc=1, device_id=device(*friend), device_id_type=MESH)
    pl.semaphore_wait(barrier, len(friends))
    for needed, load in loads:
        pl.when(needed)(load.wait)

    def quarter(h, a, k, s):
        sgn = 1 - 2 * a
        yo = place_of(y - sgn * (k * c + s * (1 - c)))
        zo = place_of(z - sgn * (k * (1 - c) + s * c))
        row, j = 2 * h + yo % 2, 2 * zo + yo // 2
        i = 2 * xs(h) + yo % 2
        here = slot(row, j, a, c)
        return here, 2 * j + c <= 2 * i + a

    diagonal = j_own == band

    def both(*conds):
        out = conds[0]
        for cond in conds[1:]:
            out = jnp.logical_and(out, cond)
        return out

    def role(values, h):
        inner_mask = jnp.where(h == 0, jnp.int32(values[0]), jnp.int32(values[1]))
        outer_mask = jnp.where(h == 0, jnp.int32(values[2]), jnp.int32(values[3]))
        return jnp.where(outer, outer_mask, inner_mask)

    def by_pair(h, k, s):
        return lax.shift_right_logical(role(BY_PAIR, h), 4 * k + s) % 2 == 1

    def both_ways(h, along_y):
        return lax.shift_right_logical(role(BOTH_WAYS, h), along_y) % 2 == 1

    def copies(h, a, k, s):
        here, real = quarter(h, a, k, s)
        sgn = 1 - 2 * a
        ours = h == h_own
        short1, short2 = both_ways(h, c), both_ways(h, 1 - c)
        ref = tiles.at[here]

        def along(m):
            return device(x, place_of(y + m * c), place_of(z + m * (1 - c)), c)

        def over(m):
            return device(x, place_of(y + m * (1 - c)), place_of(z + m * c), c)

        def ring(k2, s2):
            return both(real, jnp.logical_or(ours, jnp.logical_not(by_pair(h, k2, s2))))

        last1 = 3 - short1.astype(jnp.int32)
        last2 = 3 - short2.astype(jnp.int32)
        near = both(k == 0, s == 0)
        plan = (
            (both(real, ours, jnp.logical_or(near, by_pair(h, k, s))), device(3 - x, y, z, c)),
            (both(ring(k + 1, 0), s == 0, k < last1), along(sgn)),
            (both(ring(3, 0), near, short1), along(-sgn)),
            (both(ring(k, s + 1), s < last2), over(sgn)),
            (both(ring(k, 3), s == 0, short2), over(-sgn)),
            (real, device(x, y, z, 1 - c)),
        )
        sem = quarter_send.at[here // 2]
        return sem, [
            (cond, pltpu.make_async_remote_copy(
                src_ref=ref, dst_ref=ref, send_sem=sem, recv_sem=tile_sem.at[here],
                device_id=target, device_id_type=MESH,
            ))
            for cond, target in plan
        ]

    def finish_sends():
        for cond, copy in pending:
            if cond is None:
                copy.wait_send()
            else:
                pl.when(cond)(copy.wait_send)
        pending.clear()

    def own_quarters(ready):
        for a in range(2):
            for cond, copy in copies(h_own, a, 0, 0)[1]:
                pl.when(both(cond, ready(a)))(copy.start)

    def decode(code):
        return code // 32, code % 2, (code // 8) % 4, (code // 2) % 4

    kind = 2 * x + c

    def by_kind(values):
        out = jnp.int32(values[0])
        for n, value in enumerate(values[1:]):
            out = jnp.where(kind == n + 1, jnp.int32(value), out)
        return out

    words = [by_kind(word) for word in zip(*EVENTS)]

    def event(n, carry):
        which = n // 5
        word = words[0]
        for at, other in enumerate(words[1:]):
            word = jnp.where(which == at + 1, other, word)
        h, a, k, s = decode(lax.shift_right_logical(word, 6 * (n % 5)) % 64)
        here, real = quarter(h, a, k, s)
        pl.when(both(real, jnp.logical_not(both(h == h_own, k == 0, s == 0))))(
            lambda: arrived(tiles.at[here], tile_sem.at[here])
        )
        for cond, copy in copies(h, a, k, s)[1]:
            pl.when(cond)(copy.start)
        return carry

    def sent(code, carry):
        sem, sends = copies(*decode(code))
        number = sum(cond.astype(jnp.int32) for cond, _ in sends)
        for n in range(1, 7):
            pl.when(number == n)(lambda: arrived(tiles.at[pl.ds(0, n)], sem))
        return carry

    own_quarters(lambda a: jnp.logical_not(both(diagonal, c == a)))

    @pl.when(diagonal)
    def _():
        where = slot(place, j_own, c, c)
        rows = lax.broadcasted_iota(jnp.int32, (256, 256), 0)
        cols = lax.broadcasted_iota(jnp.int32, (256, 256), 1)
        tri = tiles[where]
        diag = jnp.where(rows == cols, tri, 0.0)
        down = 1.0 / jnp.sum(diag, axis=1, keepdims=True)
        across = 1.0 / jnp.sum(diag, axis=0, keepdims=True)
        pairs = jnp.logical_and(rows == cols + 1, rows % 2 == 1)
        inverse[...] = jnp.where(rows == cols, down, 0.0) - jnp.where(
            pairs, tri * down * across, 0.0
        )

        def level(k, carry):
            rk, ck = rows >> k, cols >> k
            inside = jnp.logical_and(rk == ck + 1, rk % 2 == 1)
            below = jnp.where(inside, tiles[where], 0.0)
            now = inverse[...]
            inverse[...] = now - product(now, product(below, now))
            return carry

        lax.fori_loop(1, 8, level, 0)
        tiles[where] = inverse[...]

    own_quarters(lambda a: both(diagonal, c == a))

    def share_rhs(when):
        for q in range(4):
            send(
                jnp.logical_and(place != q, when),
                psi.at[:, 128 * q : 128 * q + 128], rhs.at[place],
                rhs_send.at[q], rhs_sem.at[place],
                device(xs(q // 2), 2 * y_hi + q % 2, z, c),
            )

    def tile(row, j, a, b):
        return tiles[slot(row, j, a, b)]

    def from_sibling(row, j, a):
        here = slot(row, j, a, 1 - c)
        arrived(tiles.at[here], tile_sem.at[here])

    def update(row, j):
        for a in range(2):
            from_sibling(row, j, a)
        top, bottom = ys[2 * j], ys[2 * j + 1]
        for a in range(2):
            rhs[row, 256 * a : 256 * a + 256, :] = rhs[row, 256 * a : 256 * a + 256, :] - (
                narrow_product(tile(row, j, a, 0), top) + narrow_product(tile(row, j, a, 1), bottom)
            )

    def deliver(h, r, part_no):
        row = 2 * h + r
        i = 2 * xs(h) + r
        block = ys.at[2 * i + part_no]
        send(None if h == 0 else jnp.logical_not(outer), block, block,
             y_send.at[2 * row + part_no], y_sem.at[2 * i + part_no],
             device(x + 1 - 2 * (x % 2), y, z, c), False)
        send(place != row, block, owned.at[place, part_no], own_send.at[2 * row + part_no],
             own_sem.at[place, part_no], device(xs(h), 2 * y_hi + r, z, c), False)

        @pl.when(place == row)
        def _():
            owned[row, part_no] = ys[2 * i + part_no]

    def solve(h, r):
        row = 2 * h + r
        i = 2 * xs(h) + r

        @pl.when(c == 0)
        def _():
            from_sibling(row, i, 1)

        @pl.when(c == 1)
        def _():
            from_sibling(row, i, 0)
            from_sibling(row, i, 1)

        top = narrow_product(tile(row, i, 0, 0), rhs[row, 0:256, :])
        ys[2 * i] = top
        deliver(h, r, 0)
        bottom = narrow_product(
            tile(row, i, 1, 1), rhs[row, 256:512, :] - narrow_product(tile(row, i, 1, 0), top)
        )
        ys[2 * i + 1] = bottom
        deliver(h, r, 1)

    def await_rhs(h):
        for r in range(2):
            row = 2 * h + r

            @pl.when(place != row)
            def _():
                arrived(rhs.at[row], rhs_sem.at[row])

            @pl.when(place == row)
            def _():
                psi_here.wait()

    def await_y(j):
        for part_no in range(2):
            arrived(ys.at[2 * j + part_no], y_sem.at[2 * j + part_no])

    def by_columns(h, arriving):
        count = 2 * xs(h)

        def step(j, carry):
            pl.when(arriving(j))(lambda: await_y(j))
            update(2 * h, j)
            update(2 * h + 1, j)
            return carry

        lax.fori_loop(0, count, step, 0)
        solve(h, 0)
        update(2 * h + 1, count)
        solve(h, 1)

    def by_rows(h):
        count = 2 * xs(h)
        for r in range(2):
            def step(j, carry, r=r):
                update(2 * h + r, j)
                return carry

            lax.fori_loop(0, count + r, step, 0)
            solve(h, r)

    share_at, stage_at, count = by_kind(SHARE_AT), by_kind(STAGE_AT), by_kind(EVENT_COUNT)
    share_rhs(h_own == 0)
    with jax.named_scope("first"):
        lax.fori_loop(0, share_at, event, 0)
    share_rhs(h_own == 1)
    with jax.named_scope("second"):
        lax.fori_loop(share_at, stage_at, event, 0)
    with jax.named_scope("early"):
        await_rhs(0)
        by_columns(0, lambda j: jnp.logical_not(outer))
    with jax.named_scope("third"):
        lax.fori_loop(stage_at, count, event, 0)
    with jax.named_scope("last"):
        await_rhs(1)

        @pl.when(outer)
        def _():
            by_columns(1, lambda j: j >= 2)

        @pl.when(jnp.logical_not(outer))
        def _():
            by_rows(1)

    writes = []
    with jax.named_scope("product"):
        beside = place + 1 - 2 * (place % 2)
        for n, q in enumerate(
            (place, beside, lax.rem(place + 2, 4), lax.rem(beside + 2, 4))
        ):
            for a in range(2):
                if n:
                    arrived(owned.at[q, a], own_sem.at[q, a])
                write = pltpu.make_async_copy(
                    owned.at[q, a],
                    out.at[
                        256 * a : 256 * a + 256, pl.ds(pl.multiple_of(128 * q, 128), 128)
                    ],
                    local_sem.at[3 + 2 * n + a],
                )
                write.start()
                writes.append(write)
            block = owned[q].reshape(512, 128)
            at = 0
            for r in range(4):
                term = product(
                    block[128 * r : 128 * r + 128], block[: 128 * r + 128],
                    (((1,), (1,)), ((), ())),
                )
                for s in range(r + 1):
                    here = term[:, 128 * s : 128 * s + 128]
                    part[at] = here if n == 0 else part[at] + here
                    at += 1

    with jax.named_scope("halves"):
        send(None, part.at[pl.ds(5 - 5 * c, 5)], half, half_sem.at[0], half_sem.at[1],
             device(x, y, z, 1 - c))
        arrived(half, half_sem.at[1])
        half[...] = half[...] + part[pl.ds(5 * c, 5)]
    m = j_own

    def lines(of):
        return pl.ds(pl.multiple_of(16 * of, 16), 16)

    with jax.named_scope("scatter"):
        for t in range(1, 8):
            to = lax.rem(m + t, 8)
            send(None, half.at[:, lines(to)], pieces.at[t - 1],
                 rs_send.at[t - 1], rs_sem.at[t - 1],
                 device(x, 2 * (to % 2) + y_lo, to // 2, c))
        lax.fori_loop(0, 64, sent, 0)
        total = half[:, lines(m), :]
        for t in range(1, 8):
            arrived(pieces.at[t - 1], rs_sem.at[t - 1])
            total = total + pieces[t - 1]
        whole[c, :, lines(m), :] = total * (1.0 / NG)
    with jax.named_scope("spread"):
        def share(core, of, s_sem, target):
            ref = whole.at[core, :, lines(of)]
            send(None, ref, ref, s_sem, ag_sem.at[core * 8 + of], target)

        for t in range(1, 8):
            to = lax.rem(m + t, 8)
            share(c, m, ag_send.at[t - 1], device(x, 2 * (to % 2) + y_lo, to // 2, c))
        share(c, m, ag_cross.at[0], device(x, y, z, 1 - c))
        for row in range(4):
            for part_no in range(2):
                block = ys.at[2 * (2 * xs(row // 2) + row % 2) + part_no]
                sem = y_send.at[2 * row + part_no]
                if row < 2:
                    arrived(block, sem)
                else:
                    pl.when(jnp.logical_not(outer))(lambda: arrived(block, sem))
                pl.when(place != row)(lambda: arrived(block, own_send.at[2 * row + part_no]))
        for t in range(1, 8):
            of = lax.rem(m + 8 - t, 8)
            arrived(whole.at[c, :, lines(of)], ag_sem.at[c * 8 + of])
            share(c, of, ag_cross.at[t], device(x, y, z, 1 - c))
        for of in range(8):
            arrived(whole.at[1 - c, :, lines(of)], ag_sem.at[(1 - c) * 8 + of])
        at = 0
        for r in range(4):
            for s in range(r + 1):
                block = whole[at // 5, at % 5]
                inter[128 * r : 128 * r + 128, 128 * s : 128 * s + 128] = block
                if s < r:
                    inter[128 * s : 128 * s + 128, 128 * r : 128 * r + 128] = block.T
                at += 1
    finish_sends()
    for write in writes:
        write.wait()


def local(psi, lower):
    dma = pltpu.SemaphoreType.DMA
    out, inter = pl.pallas_call(
        kernel,
        out_shape=(
            pltpu.VMEM((512, 512), F32),
            pltpu.VMEM((512, 512), F32),
        ),
        in_specs=[pl.BlockSpec(memory_space=pl.ANY)] * 2,
        out_specs=(pl.BlockSpec(memory_space=pltpu.VMEM),) * 2,
        scratch_shapes=[
            pltpu.VMEM((80, 256, 256), F32),
            pltpu.VMEM((16, 256, 128), F32),
            pltpu.VMEM((4, 512, 128), F32),
            pltpu.VMEM((4, 2, 256, 128), F32),
            pltpu.VMEM((10, 128, 128), F32),
            pltpu.VMEM((5, 128, 128), F32),
            pltpu.VMEM((7, 5, 16, 128), F32),
            pltpu.VMEM((2, 5, 128, 128), F32),
            pltpu.VMEM((256, 256), F32),
            dma((80,)), dma((40,)), dma((4,)), dma((4,)),
            dma((16,)), dma((8,)), dma((4, 2)), dma((8,)), dma((2,)), dma((7,)), dma((7,)),
            dma((16,)), dma((7,)), dma((8,)), dma((12,)),
        ],
        compiler_params=pltpu.CompilerParams(
            has_side_effects=True, collective_id=0, vmem_limit_bytes=60 * 1024 * 1024
        ),
    )(psi, lower)
    return out, inter


def solution(mesh):
    return jax.shard_map(
        local,
        mesh=mesh,
        in_specs=(P("band", "ga"), P("band", "ga")),
        out_specs=(P("band", "ga"), P("band", None)),
        check_vma=False,
    )
```

```python
import jax
import jax.numpy as jnp
from jax import lax
from jax.experimental import pallas as pl
from jax.experimental.pallas import tpu as pltpu
from jax.sharding import PartitionSpec as P

MESH = pl.DeviceIdType.MESH
F32 = jnp.float32
BF16 = jnp.bfloat16
NG = 8192

EVENTS = (
    (157557187, 88368648, 457242079, 239904395, 561644356, 676684957, 475208745,
     582921100, 966683384, 600800050, 1073458605, 613899579, 3964),
    (117981848, 421847558, 437016464, 310163151, 558155168, 232879964, 346201683,
     576170672, 848280300, 1050139772, 1066617715, 668401070, 3558),
    (538452489, 256250307, 388804112, 963021390, 373915987, 833331981, 998967492,
     447608085, 1016458395, 762466156, 1067378547, 1052727732, 3574),
    (50890272, 68556361, 102545034, 642103824, 204874921, 495832100, 666547155,
     830008298, 364008735, 937921398, 854158551, 1037262590, 4092),
    (10717347, 815241793, 837460516, 61673161, 843412678, 172650631, 1039321523,
     423285464, 773014927, 892858335, 439375125, 477063087, 1911),
    (637704360, 404912321, 616583406, 46076202, 174765669, 270039881, 971205874,
     455919452, 290421522, 528219445, 339460026, 401695573, 3919),
    (157548611, 678196744, 324966539, 591032998, 812194895, 36980550, 524363077,
     954517270, 514517743, 865160677, 771714738, 886565691, 3964),
    (135794816, 51671310, 589966888, 417641434, 304453979, 207262756, 300801706,
     508614620, 761166891, 1011817254, 365882557, 901730302, 3574),
)
SHARE_AT = (14, 13, 42, 41, 43, 46, 15, 19)
STAGE_AT = (38, 42, 52, 56, 62, 62, 51, 62)
EVENT_COUNT = (62, 62, 62, 62, 62, 62, 62, 62)
BY_PAIR = ((51726, 51726), (526, 526), (32510, 32510), (14, 14))
BOTH_WAYS = ((2, 2), (1, 1), (3, 3), (2, 2))


def split(a):
    high = a.astype(BF16)
    return high, (a - high.astype(F32)).astype(BF16)


def product(a, b):
    ah, al = split(a)
    bh, bl = split(b)

    def dot(p, q):
        return jnp.dot(p, q, preferred_element_type=F32)

    return dot(ah, bh) + (dot(ah, bl) + dot(al, bh))


def outer_product(a, b):
    ah, al = split(a)
    bh, bl = split(b)

    def dot(p, q):
        return lax.dot_general(p, q, (((1,), (1,)), ((), ())), preferred_element_type=F32)

    return dot(ah, bl) + dot(
        jnp.concatenate([ah, al], axis=1), jnp.concatenate([bh, bh], axis=1)
    )


def narrow_product(a, b):
    ah, al = split(a)
    bh, bl = split(b)
    wide = jnp.dot(ah, jnp.concatenate([bh, bl], axis=1), preferred_element_type=F32)
    rest = jnp.dot(al, bh, preferred_element_type=F32)
    return wide[:, :128] + (wide[:, 128:] + rest)


def kernel(
    psi, lower, out, inter,
    tiles, ys, rhs, owned, part, half, pieces, whole, inverse,
    tile_sem, quarter_send, rhs_sem, rhs_send,
    y_sem, y_send, own_sem, own_send, half_sem, rs_sem, rs_send, ag_sem, ag_send,
    ag_cross, local_sem,
):
    band = lax.axis_index("band")
    ga = lax.axis_index("ga")
    x, y_lo = band // 2, band % 2
    z, y_hi, c = ga // 4, (ga // 2) % 2, ga % 2
    y = 2 * y_hi + y_lo
    h_own = x // 2
    outer = jnp.logical_or(x == 0, x == 3)
    x_low = jnp.minimum(x, 3 - x)
    place = 2 * h_own + y_lo

    def device(dx, dy, dz, dc):
        return (2 * dx + dy % 2, 4 * dz + 2 * (dy // 2) + dc)

    def xs(h):
        return x_low * (1 - h) + (3 - x_low) * h

    low, high = 2 * x_low, 2 * (3 - x_low)

    def slot(row, j, a, b):
        before = jnp.where(row > 0, low + 1, 0) + jnp.where(row > 1, low + 2, 0)
        before = before + jnp.where(row > 2, high + 1, 0)
        return ((before + j) * 2 + a) * 2 + b

    pending = []

    def send(cond, src, dst, s_sem, r_sem, target, later=True):
        copy = pltpu.make_async_remote_copy(
            src_ref=src, dst_ref=dst, send_sem=s_sem, recv_sem=r_sem,
            device_id=target, device_id_type=MESH,
        )
        if cond is None:
            copy.start()
        else:
            pl.when(cond)(copy.start)
        if later:
            pending.append((cond, copy))
        return copy

    def arrived(ref, sem):
        pltpu.make_async_copy(ref, ref, sem).wait()

    j_own = 2 * z + y_hi
    loads = []
    for a in range(2):
        load = pltpu.make_async_copy(
            lower.at[256 * a : 256 * a + 256, :], tiles.at[slot(place, j_own, a, c)],
            local_sem.at[1 + a],
        )
        needed = 2 * j_own + c <= 2 * band + a
        pl.when(needed)(load.start)
        loads.append((needed, load))
    psi_here = pltpu.make_async_copy(
        psi.at[:, pl.ds(pl.multiple_of(128 * place, 128), 128)], rhs.at[place], local_sem.at[0]
    )
    psi_here.start()

    def place_of(v):
        return lax.rem(v + 8, 4)

    barrier = pltpu.get_barrier_semaphore()
    friends = [
        (3 - x, y, z, c), (x, 2 * y_hi + 1 - y_lo, z, c), (3 - x, 2 * y_hi + 1 - y_lo, z, c),
        (x + 1 - 2 * (x % 2), y, z, c), (x, y, z, 1 - c),
        (x, place_of(y + 1), z, c), (x, place_of(y - 1), z, c),
        (x, y, place_of(z + 1), c), (x, y, place_of(z - 1), c),
    ] + [
        (x, 2 * (lax.rem(j_own + t, 8) % 2) + y_lo, lax.rem(j_own + t, 8) // 2, c)
        for t in range(1, 8)
    ]
    for friend in friends:
        pl.semaphore_signal(barrier, inc=1, device_id=device(*friend), device_id_type=MESH)
    pl.semaphore_wait(barrier, len(friends))
    for needed, load in loads:
        pl.when(needed)(load.wait)

    def quarter(h, a, k, s):
        sgn = 1 - 2 * a
        yo = place_of(y - sgn * (k * c + s * (1 - c)))
        zo = place_of(z - sgn * (k * (1 - c) + s * c))
        row, j = 2 * h + yo % 2, 2 * zo + yo // 2
        i = 2 * xs(h) + yo % 2
        here = slot(row, j, a, c)
        return here, 2 * j + c <= 2 * i + a

    diagonal = j_own == band

    def both(*conds):
        out = conds[0]
        for cond in conds[1:]:
            out = jnp.logical_and(out, cond)
        return out

    def role(values, h):
        of = [jnp.where(c == 0, jnp.int32(a), jnp.int32(b)) for a, b in values]
        return jnp.where(
            outer, jnp.where(h == 0, of[2], of[3]), jnp.where(h == 0, of[0], of[1])
        )

    def by_pair(h, k, s):
        return lax.shift_right_logical(role(BY_PAIR, h), 4 * k + s) % 2 == 1

    def both_ways(h, along_y):
        return lax.shift_right_logical(role(BOTH_WAYS, h), along_y) % 2 == 1

    def copies(h, a, k, s):
        here, real = quarter(h, a, k, s)
        sgn = 1 - 2 * a
        ours = h == h_own
        short1, short2 = both_ways(h, c), both_ways(h, 1 - c)
        ref = tiles.at[here]

        def along(m):
            return device(x, place_of(y + m * c), place_of(z + m * (1 - c)), c)

        def over(m):
            return device(x, place_of(y + m * (1 - c)), place_of(z + m * c), c)

        def ring(k2, s2):
            return both(real, jnp.logical_or(ours, jnp.logical_not(by_pair(h, k2, s2))))

        last1 = 3 - short1.astype(jnp.int32)
        last2 = 3 - short2.astype(jnp.int32)
        near = both(k == 0, s == 0)
        plan = (
            (both(real, ours, jnp.logical_or(near, by_pair(h, k, s))), device(3 - x, y, z, c)),
            (both(ring(k + 1, 0), s == 0, k < last1), along(sgn)),
            (both(ring(3, 0), near, short1), along(-sgn)),
            (both(ring(k, s + 1), s < last2), over(sgn)),
            (both(ring(k, 3), s == 0, short2), over(-sgn)),
            (real, device(x, y, z, 1 - c)),
        )
        sem = quarter_send.at[here // 2]
        return sem, [
            (cond, pltpu.make_async_remote_copy(
                src_ref=ref, dst_ref=ref, send_sem=sem, recv_sem=tile_sem.at[here],
                device_id=target, device_id_type=MESH,
            ))
            for cond, target in plan
        ]

    def finish_sends():
        for cond, copy in pending:
            if cond is None:
                copy.wait_send()
            else:
                pl.when(cond)(copy.wait_send)
        pending.clear()

    def own_quarters(ready):
        for a in range(2):
            for cond, copy in copies(h_own, a, 0, 0)[1]:
                pl.when(both(cond, ready(a)))(copy.start)

    def decode(code):
        return code // 32, code % 2, (code // 8) % 4, (code // 2) % 4

    kind = 2 * x + c

    def by_kind(values):
        out = jnp.int32(values[0])
        for n, value in enumerate(values[1:]):
            out = jnp.where(kind == n + 1, jnp.int32(value), out)
        return out

    words = [by_kind(word) for word in zip(*EVENTS)]

    def event(n, carry):
        which = n // 5
        word = words[0]
        for at, other in enumerate(words[1:]):
            word = jnp.where(which == at + 1, other, word)
        h, a, k, s = decode(lax.shift_right_logical(word, 6 * (n % 5)) % 64)
        here, real = quarter(h, a, k, s)
        pl.when(both(real, jnp.logical_not(both(h == h_own, k == 0, s == 0))))(
            lambda: arrived(tiles.at[here], tile_sem.at[here])
        )
        for cond, copy in copies(h, a, k, s)[1]:
            pl.when(cond)(copy.start)
        return carry

    def sent(code, carry):
        sem, sends = copies(*decode(code))
        number = sum(cond.astype(jnp.int32) for cond, _ in sends)
        for n in range(1, 7):
            pl.when(number == n)(lambda: arrived(tiles.at[pl.ds(0, n)], sem))
        return carry

    own_quarters(lambda a: jnp.logical_not(both(diagonal, c == a)))

    @pl.when(diagonal)
    def _():
        where = slot(place, j_own, c, c)
        rows = lax.broadcasted_iota(jnp.int32, (256, 256), 0)
        cols = lax.broadcasted_iota(jnp.int32, (256, 256), 1)
        tri = tiles[where]
        diag = jnp.where(rows == cols, tri, 0.0)
        down = 1.0 / jnp.sum(diag, axis=1, keepdims=True)
        across = 1.0 / jnp.sum(diag, axis=0, keepdims=True)
        pairs = jnp.logical_and(rows == cols + 1, rows % 2 == 1)
        inverse[...] = jnp.where(rows == cols, down, 0.0) - jnp.where(
            pairs, tri * down * across, 0.0
        )

        def level(k, carry):
            rk, ck = rows >> k, cols >> k
            inside = jnp.logical_and(rk == ck + 1, rk % 2 == 1)
            below = jnp.where(inside, tiles[where], 0.0)
            now = inverse[...]
            inverse[...] = now - product(now, product(below, now))
            return carry

        lax.fori_loop(1, 8, level, 0)
        tiles[where] = inverse[...]

    own_quarters(lambda a: both(diagonal, c == a))

    def share_rhs(when):
        for q in range(4):
            send(
                jnp.logical_and(place != q, when),
                psi.at[:, 128 * q : 128 * q + 128], rhs.at[place],
                rhs_send.at[q], rhs_sem.at[place],
                device(xs(q // 2), 2 * y_hi + q % 2, z, c),
            )

    def tile(row, j, a, b):
        return tiles[slot(row, j, a, b)]

    def from_sibling(row, j, a):
        here = slot(row, j, a, 1 - c)
        arrived(tiles.at[here], tile_sem.at[here])

    def update(row, j):
        for a in range(2):
            from_sibling(row, j, a)
        top, bottom = ys[2 * j], ys[2 * j + 1]
        for a in range(2):
            rhs[row, 256 * a : 256 * a + 256, :] = rhs[row, 256 * a : 256 * a + 256, :] - (
                narrow_product(tile(row, j, a, 0), top) + narrow_product(tile(row, j, a, 1), bottom)
            )

    def deliver(h, r, part_no):
        row = 2 * h + r
        i = 2 * xs(h) + r
        block = ys.at[2 * i + part_no]
        send(None if h == 0 else jnp.logical_not(outer), block, block,
             y_send.at[2 * row + part_no], y_sem.at[2 * i + part_no],
             device(x + 1 - 2 * (x % 2), y, z, c), False)
        send(place != row, block, owned.at[place, part_no], own_send.at[2 * row + part_no],
             own_sem.at[place, part_no], device(xs(h), 2 * y_hi + r, z, c), False)

        @pl.when(place == row)
        def _():
            owned[row, part_no] = ys[2 * i + part_no]

    def solve(h, r):
        row = 2 * h + r
        i = 2 * xs(h) + r

        @pl.when(c == 0)
        def _():
            from_sibling(row, i, 1)

        @pl.when(c == 1)
        def _():
            from_sibling(row, i, 0)
            from_sibling(row, i, 1)

        top = narrow_product(tile(row, i, 0, 0), rhs[row, 0:256, :])
        ys[2 * i] = top
        deliver(h, r, 0)
        bottom = narrow_product(
            tile(row, i, 1, 1), rhs[row, 256:512, :] - narrow_product(tile(row, i, 1, 0), top)
        )
        ys[2 * i + 1] = bottom
        deliver(h, r, 1)

    def await_rhs(h):
        for r in range(2):
            row = 2 * h + r

            @pl.when(place != row)
            def _():
                arrived(rhs.at[row], rhs_sem.at[row])

            @pl.when(place == row)
            def _():
                psi_here.wait()

    def await_y(j):
        for part_no in range(2):
            arrived(ys.at[2 * j + part_no], y_sem.at[2 * j + part_no])

    def by_columns(h, arriving):
        count = 2 * xs(h)

        def step(j, carry):
            pl.when(arriving(j))(lambda: await_y(j))
            update(2 * h, j)
            update(2 * h + 1, j)
            return carry

        lax.fori_loop(0, count, step, 0)
        solve(h, 0)
        update(2 * h + 1, count)
        solve(h, 1)

    def by_rows(h):
        count = 2 * xs(h)
        for r in range(2):
            def step(j, carry, r=r):
                update(2 * h + r, j)
                return carry

            lax.fori_loop(0, count + r, step, 0)
            solve(h, r)

    share_at, stage_at, count = by_kind(SHARE_AT), by_kind(STAGE_AT), by_kind(EVENT_COUNT)
    share_rhs(h_own == 0)
    with jax.named_scope("first"):
        lax.fori_loop(0, share_at, event, 0)
    share_rhs(h_own == 1)
    with jax.named_scope("second"):
        lax.fori_loop(share_at, stage_at, event, 0)
    with jax.named_scope("early"):
        await_rhs(0)
        by_columns(0, lambda j: jnp.logical_not(outer))
    with jax.named_scope("third"):
        lax.fori_loop(stage_at, count, event, 0)
    with jax.named_scope("last"):
        await_rhs(1)

        @pl.when(outer)
        def _():
            by_columns(1, lambda j: j >= 2)

        @pl.when(jnp.logical_not(outer))
        def _():
            by_rows(1)

    writes = []
    with jax.named_scope("product"):
        beside = place + 1 - 2 * (place % 2)
        for n, q in enumerate(
            (place, beside, lax.rem(place + 2, 4), lax.rem(beside + 2, 4))
        ):
            for a in range(2):
                if n:
                    arrived(owned.at[q, a], own_sem.at[q, a])
                write = pltpu.make_async_copy(
                    owned.at[q, a],
                    out.at[
                        256 * a : 256 * a + 256, pl.ds(pl.multiple_of(128 * q, 128), 128)
                    ],
                    local_sem.at[3 + 2 * n + a],
                )
                write.start()
                writes.append(write)
            block = owned[q].reshape(512, 128)
            at = 0
            for r in range(4):
                term = outer_product(
                    block[128 * r : 128 * r + 128], block[: 128 * r + 128]
                )
                for s in range(r + 1):
                    here = term[:, 128 * s : 128 * s + 128]
                    part[at] = here if n == 0 else part[at] + here
                    at += 1

    with jax.named_scope("halves"):
        send(None, part.at[pl.ds(5 - 5 * c, 5)], half, half_sem.at[0], half_sem.at[1],
             device(x, y, z, 1 - c))
        arrived(half, half_sem.at[1])
        half[...] = half[...] + part[pl.ds(5 * c, 5)]
    m = j_own

    def lines(of):
        return pl.ds(pl.multiple_of(16 * of, 16), 16)

    with jax.named_scope("scatter"):
        for t in range(1, 8):
            to = lax.rem(m + t, 8)
            send(None, half.at[:, lines(to)], pieces.at[t - 1],
                 rs_send.at[t - 1], rs_sem.at[t - 1],
                 device(x, 2 * (to % 2) + y_lo, to // 2, c))
        lax.fori_loop(0, 64, sent, 0)
        total = half[:, lines(m), :]
        for t in range(1, 8):
            arrived(pieces.at[t - 1], rs_sem.at[t - 1])
            total = total + pieces[t - 1]
        whole[c, :, lines(m), :] = total * (1.0 / NG)
    with jax.named_scope("spread"):
        def share(core, of, s_sem, target):
            ref = whole.at[core, :, lines(of)]
            send(None, ref, ref, s_sem, ag_sem.at[core * 8 + of], target)

        for t in range(1, 8):
            to = lax.rem(m + t, 8)
            share(c, m, ag_send.at[t - 1], device(x, 2 * (to % 2) + y_lo, to // 2, c))
        share(c, m, ag_cross.at[0], device(x, y, z, 1 - c))
        for row in range(4):
            for part_no in range(2):
                block = ys.at[2 * (2 * xs(row // 2) + row % 2) + part_no]
                sem = y_send.at[2 * row + part_no]
                if row < 2:
                    arrived(block, sem)
                else:
                    pl.when(jnp.logical_not(outer))(lambda: arrived(block, sem))
                pl.when(place != row)(lambda: arrived(block, own_send.at[2 * row + part_no]))
        for t in range(1, 8):
            of = lax.rem(m + 8 - t, 8)
            arrived(whole.at[c, :, lines(of)], ag_sem.at[c * 8 + of])
            share(c, of, ag_cross.at[t], device(x, y, z, 1 - c))
        for of in range(8):
            arrived(whole.at[1 - c, :, lines(of)], ag_sem.at[(1 - c) * 8 + of])
        at = 0
        for r in range(4):
            for s in range(r + 1):
                block = whole[at // 5, at % 5]
                inter[128 * r : 128 * r + 128, 128 * s : 128 * s + 128] = block
                if s < r:
                    inter[128 * s : 128 * s + 128, 128 * r : 128 * r + 128] = block.T
                at += 1
    finish_sends()
    for write in writes:
        write.wait()


def local(psi, lower):
    dma = pltpu.SemaphoreType.DMA
    out, inter = pl.pallas_call(
        kernel,
        out_shape=(
            pltpu.VMEM((512, 512), F32),
            pltpu.VMEM((512, 512), F32),
        ),
        in_specs=[pl.BlockSpec(memory_space=pl.ANY)] * 2,
        out_specs=(pl.BlockSpec(memory_space=pltpu.VMEM),) * 2,
        scratch_shapes=[
            pltpu.VMEM((80, 256, 256), F32),
            pltpu.VMEM((16, 256, 128), F32),
            pltpu.VMEM((4, 512, 128), F32),
            pltpu.VMEM((4, 2, 256, 128), F32),
            pltpu.VMEM((10, 128, 128), F32),
            pltpu.VMEM((5, 128, 128), F32),
            pltpu.VMEM((7, 5, 16, 128), F32),
            pltpu.VMEM((2, 5, 128, 128), F32),
            pltpu.VMEM((256, 256), F32),
            dma((80,)), dma((40,)), dma((4,)), dma((4,)),
            dma((16,)), dma((8,)), dma((4, 2)), dma((8,)), dma((2,)), dma((7,)), dma((7,)),
            dma((16,)), dma((7,)), dma((8,)), dma((12,)),
        ],
        compiler_params=pltpu.CompilerParams(
            has_side_effects=True, collective_id=0, vmem_limit_bytes=60 * 1024 * 1024
        ),
    )(psi, lower)
    return out, inter


def solution(mesh):
    return jax.shard_map(
        local,
        mesh=mesh,
        in_specs=(P("band", "ga"), P("band", "ga")),
        out_specs=(P("band", "ga"), P("band", None)),
        check_vma=False,
    )
```

```python
import jax
import jax.numpy as jnp
from jax import lax
from jax.experimental import pallas as pl
from jax.experimental.pallas import tpu as pltpu
from jax.sharding import PartitionSpec as P

MESH = pl.DeviceIdType.MESH
F32 = jnp.float32
BF16 = jnp.bfloat16
NG = 8192

EVENTS = (
    (35402841, 403997254, 191693791, 239968919, 511824708, 362898593, 834718300,
     948628116, 849059307, 663669747, 1072426413, 1016552763, 2365),
    (102506776, 174338574, 438589328, 523088850, 558155168, 685864796, 816289043,
     576168810, 602917612, 634379185, 1066659122, 664493037, 3511),
    (538452489, 273027523, 675118633, 962912907, 206143827, 602649430, 806557866,
     447608085, 1016481691, 768200556, 668198771, 802581439, 3511),
    (56754690, 68556361, 102539994, 642103824, 227093068, 328117276, 666520271,
     836365277, 626060117, 931110444, 845129139, 886570750, 3901),
    (31598824, 143658601, 720046449, 101519049, 35595371, 754398439, 1012818578,
     255513304, 336698646, 1062600622, 439375797, 930308975, 1883),
    (25848384, 86145256, 814758808, 78270635, 182033393, 152857754, 313854771,
     493735544, 215293387, 1073431443, 351250398, 1012495189, 1021),
    (392429635, 463831561, 322577128, 597469575, 488182769, 96596804, 380458138,
     791909378, 514516792, 848509268, 1052209146, 1039096631, 3388),
    (135798785, 940339470, 589965829, 304936633, 270947928, 464045481, 474339643,
     339113978, 398584235, 1011817261, 365882557, 920080382, 3063),
)
SHARE_AT = (13, 13, 41, 34, 35, 44, 15, 15)
STAGE_AT = (38, 42, 52, 56, 62, 62, 51, 61)
EVENT_COUNT = (62, 62, 62, 62, 62, 62, 62, 62)
BY_PAIR = ((51726, 51726), (526, 526), (32510, 32510), (14, 14))
BOTH_WAYS = ((2, 2), (1, 1), (3, 3), (2, 2))


def split(a):
    high = a.astype(BF16)
    return high, (a - high.astype(F32)).astype(BF16)


def product(a, b):
    ah, al = split(a)
    bh, bl = split(b)

    def dot(p, q):
        return jnp.dot(p, q, preferred_element_type=F32)

    return dot(ah, bh) + (dot(ah, bl) + dot(al, bh))


def outer_product(a, b):
    ah, al = split(a)
    bh, bl = split(b)

    def dot(p, q):
        return lax.dot_general(p, q, (((1,), (1,)), ((), ())), preferred_element_type=F32)

    return dot(ah, bl) + dot(
        jnp.concatenate([ah, al], axis=1), jnp.concatenate([bh, bh], axis=1)
    )


def narrow_product(a, b):
    ah, al = split(a)
    bh, bl = split(b)
    wide = jnp.dot(ah, jnp.concatenate([bh, bl], axis=1), preferred_element_type=F32)
    rest = jnp.dot(al, bh, preferred_element_type=F32)
    return wide[:, :128] + (wide[:, 128:] + rest)


def kernel(
    psi, lower, out, inter,
    tiles, ys, rhs, owned, part, half, pieces, whole, inverse,
    tile_sem, quarter_send, rhs_sem, rhs_send,
    y_sem, y_send, own_sem, own_send, half_sem, rs_sem, rs_send, ag_sem, ag_send,
    ag_cross, local_sem,
):
    band = lax.axis_index("band")
    ga = lax.axis_index("ga")
    x, y_lo = band // 2, band % 2
    z, y_hi, c = ga // 4, (ga // 2) % 2, ga % 2
    y = 2 * y_hi + y_lo
    h_own = x // 2
    outer = jnp.logical_or(x == 0, x == 3)
    x_low = jnp.minimum(x, 3 - x)
    place = 2 * h_own + y_lo

    def device(dx, dy, dz, dc):
        return (2 * dx + dy % 2, 4 * dz + 2 * (dy // 2) + dc)

    def xs(h):
        return x_low * (1 - h) + (3 - x_low) * h

    low, high = 2 * x_low, 2 * (3 - x_low)

    def slot(row, j, a, b):
        before = jnp.where(row > 0, low + 1, 0) + jnp.where(row > 1, low + 2, 0)
        before = before + jnp.where(row > 2, high + 1, 0)
        return ((before + j) * 2 + a) * 2 + b

    pending = []

    def send(cond, src, dst, s_sem, r_sem, target, later=True):
        copy = pltpu.make_async_remote_copy(
            src_ref=src, dst_ref=dst, send_sem=s_sem, recv_sem=r_sem,
            device_id=target, device_id_type=MESH,
        )
        if cond is None:
            copy.start()
        else:
            pl.when(cond)(copy.start)
        if later:
            pending.append((cond, copy))
        return copy

    def arrived(ref, sem):
        pltpu.make_async_copy(ref, ref, sem).wait()

    j_own = 2 * z + y_hi
    loads = []
    for a in range(2):
        load = pltpu.make_async_copy(
            lower.at[256 * a : 256 * a + 256, :], tiles.at[slot(place, j_own, a, c)],
            local_sem.at[1 + a],
        )
        needed = 2 * j_own + c <= 2 * band + a
        pl.when(needed)(load.start)
        loads.append((needed, load))
    psi_here = pltpu.make_async_copy(
        psi.at[:, pl.ds(pl.multiple_of(128 * place, 128), 128)], rhs.at[place], local_sem.at[0]
    )
    psi_here.start()

    def place_of(v):
        return lax.rem(v + 8, 4)

    barrier = pltpu.get_barrier_semaphore()
    friends = [
        (3 - x, y, z, c), (x, 2 * y_hi + 1 - y_lo, z, c), (3 - x, 2 * y_hi + 1 - y_lo, z, c),
        (x + 1 - 2 * (x % 2), y, z, c), (x, y, z, 1 - c),
        (x, place_of(y + 1), z, c), (x, place_of(y - 1), z, c),
        (x, y, place_of(z + 1), c), (x, y, place_of(z - 1), c),
    ] + [
        (x, 2 * (lax.rem(j_own + t, 8) % 2) + y_lo, lax.rem(j_own + t, 8) // 2, c)
        for t in range(1, 8)
    ]
    for friend in friends:
        pl.semaphore_signal(barrier, inc=1, device_id=device(*friend), device_id_type=MESH)
    pl.semaphore_wait(barrier, len(friends))
    for needed, load in loads:
        pl.when(needed)(load.wait)

    def quarter(h, a, k, s):
        sgn = 1 - 2 * a
        yo = place_of(y - sgn * (k * c + s * (1 - c)))
        zo = place_of(z - sgn * (k * (1 - c) + s * c))
        row, j = 2 * h + yo % 2, 2 * zo + yo // 2
        i = 2 * xs(h) + yo % 2
        here = slot(row, j, a, c)
        return here, 2 * j + c <= 2 * i + a

    diagonal = j_own == band

    def both(*conds):
        out = conds[0]
        for cond in conds[1:]:
            out = jnp.logical_and(out, cond)
        return out

    def role(values, h):
        of = [jnp.where(c == 0, jnp.int32(a), jnp.int32(b)) for a, b in values]
        return jnp.where(
            outer, jnp.where(h == 0, of[2], of[3]), jnp.where(h == 0, of[0], of[1])
        )

    def by_pair(h, k, s):
        return lax.shift_right_logical(role(BY_PAIR, h), 4 * k + s) % 2 == 1

    def both_ways(h, along_y):
        return lax.shift_right_logical(role(BOTH_WAYS, h), along_y) % 2 == 1

    def copies(h, a, k, s):
        here, real = quarter(h, a, k, s)
        sgn = 1 - 2 * a
        ours = h == h_own
        short1, short2 = both_ways(h, c), both_ways(h, 1 - c)
        ref = tiles.at[here]

        def along(m):
            return device(x, place_of(y + m * c), place_of(z + m * (1 - c)), c)

        def over(m):
            return device(x, place_of(y + m * (1 - c)), place_of(z + m * c), c)

        def ring(k2, s2):
            return both(real, jnp.logical_or(ours, jnp.logical_not(by_pair(h, k2, s2))))

        last1 = 3 - short1.astype(jnp.int32)
        last2 = 3 - short2.astype(jnp.int32)
        near = both(k == 0, s == 0)
        plan = (
            (both(real, ours, jnp.logical_or(near, by_pair(h, k, s))), device(3 - x, y, z, c)),
            (both(ring(k + 1, 0), s == 0, k < last1), along(sgn)),
            (both(ring(3, 0), near, short1), along(-sgn)),
            (both(ring(k, s + 1), s < last2), over(sgn)),
            (both(ring(k, 3), s == 0, short2), over(-sgn)),
            (real, device(x, y, z, 1 - c)),
        )
        sem = quarter_send.at[here // 2]
        return sem, [
            (cond, pltpu.make_async_remote_copy(
                src_ref=ref, dst_ref=ref, send_sem=sem, recv_sem=tile_sem.at[here],
                device_id=target, device_id_type=MESH,
            ))
            for cond, target in plan
        ]

    def finish_sends():
        for cond, copy in pending:
            if cond is None:
                copy.wait_send()
            else:
                pl.when(cond)(copy.wait_send)
        pending.clear()

    def own_quarters(ready):
        for a in range(2):
            for cond, copy in copies(h_own, a, 0, 0)[1]:
                pl.when(both(cond, ready(a)))(copy.start)

    def decode(code):
        return code // 32, code % 2, (code // 8) % 4, (code // 2) % 4

    kind = 2 * x + c

    def by_kind(values):
        out = jnp.int32(values[0])
        for n, value in enumerate(values[1:]):
            out = jnp.where(kind == n + 1, jnp.int32(value), out)
        return out

    words = [by_kind(word) for word in zip(*EVENTS)]

    def event(n, carry):
        which = n // 5
        word = words[0]
        for at, other in enumerate(words[1:]):
            word = jnp.where(which == at + 1, other, word)
        h, a, k, s = decode(lax.shift_right_logical(word, 6 * (n % 5)) % 64)
        here, real = quarter(h, a, k, s)
        pl.when(both(real, jnp.logical_not(both(h == h_own, k == 0, s == 0))))(
            lambda: arrived(tiles.at[here], tile_sem.at[here])
        )
        for cond, copy in copies(h, a, k, s)[1]:
            pl.when(cond)(copy.start)
        return carry

    def sent(code, carry):
        sem, sends = copies(*decode(code))
        number = sum(cond.astype(jnp.int32) for cond, _ in sends)
        for n in range(1, 7):
            pl.when(number == n)(lambda: arrived(tiles.at[pl.ds(0, n)], sem))
        return carry

    own_quarters(lambda a: jnp.logical_not(both(diagonal, c == a)))

    @pl.when(diagonal)
    def _():
        where = slot(place, j_own, c, c)
        rows = lax.broadcasted_iota(jnp.int32, (256, 256), 0)
        cols = lax.broadcasted_iota(jnp.int32, (256, 256), 1)
        tri = tiles[where]
        diag = jnp.where(rows == cols, tri, 0.0)
        down = 1.0 / jnp.sum(diag, axis=1, keepdims=True)
        across = 1.0 / jnp.sum(diag, axis=0, keepdims=True)
        pairs = jnp.logical_and(rows == cols + 1, rows % 2 == 1)
        inverse[...] = jnp.where(rows == cols, down, 0.0) - jnp.where(
            pairs, tri * down * across, 0.0
        )

        def level(k, carry):
            rk, ck = rows >> k, cols >> k
            inside = jnp.logical_and(rk == ck + 1, rk % 2 == 1)
            below = jnp.where(inside, tiles[where], 0.0)
            now = inverse[...]
            inverse[...] = now - product(now, product(below, now))
            return carry

        lax.fori_loop(1, 8, level, 0)
        tiles[where] = inverse[...]

    own_quarters(lambda a: both(diagonal, c == a))

    def share_rhs(when):
        for q in range(4):
            send(
                jnp.logical_and(place != q, when),
                psi.at[:, 128 * q : 128 * q + 128], rhs.at[place],
                rhs_send.at[q], rhs_sem.at[place],
                device(xs(q // 2), 2 * y_hi + q % 2, z, c),
            )

    def tile(row, j, a, b):
        return tiles[slot(row, j, a, b)]

    def from_sibling(row, j, a):
        here = slot(row, j, a, 1 - c)
        arrived(tiles.at[here], tile_sem.at[here])

    def update(row, j):
        for a in range(2):
            from_sibling(row, j, a)
        top, bottom = ys[2 * j], ys[2 * j + 1]
        for a in range(2):
            rhs[row, 256 * a : 256 * a + 256, :] = rhs[row, 256 * a : 256 * a + 256, :] - (
                narrow_product(tile(row, j, a, 0), top) + narrow_product(tile(row, j, a, 1), bottom)
            )

    def deliver(h, r, part_no):
        row = 2 * h + r
        i = 2 * xs(h) + r
        block = ys.at[2 * i + part_no]
        send(None if h == 0 else jnp.logical_not(outer), block, block,
             y_send.at[2 * row + part_no], y_sem.at[2 * i + part_no],
             device(x + 1 - 2 * (x % 2), y, z, c), False)
        send(place != row, block, owned.at[place, part_no], own_send.at[2 * row + part_no],
             own_sem.at[place, part_no], device(xs(h), 2 * y_hi + r, z, c), False)

        @pl.when(place == row)
        def _():
            owned[row, part_no] = ys[2 * i + part_no]

    def solve(h, r):
        row = 2 * h + r
        i = 2 * xs(h) + r

        @pl.when(c == 0)
        def _():
            from_sibling(row, i, 1)

        @pl.when(c == 1)
        def _():
            from_sibling(row, i, 0)
            from_sibling(row, i, 1)

        top = narrow_product(tile(row, i, 0, 0), rhs[row, 0:256, :])
        ys[2 * i] = top
        deliver(h, r, 0)
        bottom = narrow_product(
            tile(row, i, 1, 1), rhs[row, 256:512, :] - narrow_product(tile(row, i, 1, 0), top)
        )
        ys[2 * i + 1] = bottom
        deliver(h, r, 1)

    def await_rhs(h):
        for r in range(2):
            row = 2 * h + r

            @pl.when(place != row)
            def _():
                arrived(rhs.at[row], rhs_sem.at[row])

            @pl.when(place == row)
            def _():
                psi_here.wait()

    def await_y(j):
        for part_no in range(2):
            arrived(ys.at[2 * j + part_no], y_sem.at[2 * j + part_no])

    def by_columns(h, arriving):
        count = 2 * xs(h)

        def step(j, carry):
            pl.when(arriving(j))(lambda: await_y(j))
            update(2 * h, j)
            update(2 * h + 1, j)
            return carry

        lax.fori_loop(0, count, step, 0)
        solve(h, 0)
        update(2 * h + 1, count)
        solve(h, 1)

    def by_rows(h):
        count = 2 * xs(h)
        for r in range(2):
            def step(j, carry, r=r):
                update(2 * h + r, j)
                return carry

            lax.fori_loop(0, count + r, step, 0)
            solve(h, r)

    share_at, stage_at, count = by_kind(SHARE_AT), by_kind(STAGE_AT), by_kind(EVENT_COUNT)
    share_rhs(h_own == 0)
    with jax.named_scope("first"):
        lax.fori_loop(0, share_at, event, 0)
    share_rhs(h_own == 1)
    with jax.named_scope("second"):
        lax.fori_loop(share_at, stage_at, event, 0)
    with jax.named_scope("early"):
        await_rhs(0)
        by_columns(0, lambda j: jnp.logical_not(outer))
    with jax.named_scope("third"):
        lax.fori_loop(stage_at, count, event, 0)
    with jax.named_scope("last"):
        await_rhs(1)

        @pl.when(outer)
        def _():
            by_columns(1, lambda j: j >= 2)

        @pl.when(jnp.logical_not(outer))
        def _():
            by_rows(1)

    writes = []
    with jax.named_scope("product"):
        beside = place + 1 - 2 * (place % 2)
        for n, q in enumerate(
            (place, beside, lax.rem(place + 2, 4), lax.rem(beside + 2, 4))
        ):
            for a in range(2):
                if n:
                    arrived(owned.at[q, a], own_sem.at[q, a])
                write = pltpu.make_async_copy(
                    owned.at[q, a],
                    out.at[
                        256 * a : 256 * a + 256, pl.ds(pl.multiple_of(128 * q, 128), 128)
                    ],
                    local_sem.at[3 + 2 * n + a],
                )
                write.start()
                writes.append(write)
            block = owned[q].reshape(512, 128)
            at = 0
            for r in range(4):
                term = outer_product(
                    block[128 * r : 128 * r + 128], block[: 128 * r + 128]
                )
                for s in range(r + 1):
                    here = term[:, 128 * s : 128 * s + 128]
                    part[at] = here if n == 0 else part[at] + here
                    at += 1

    with jax.named_scope("halves"):
        send(None, part.at[pl.ds(5 - 5 * c, 5)], half, half_sem.at[0], half_sem.at[1],
             device(x, y, z, 1 - c))
        arrived(half, half_sem.at[1])
        half[...] = half[...] + part[pl.ds(5 * c, 5)]
    m = j_own

    def lines(of):
        return pl.ds(pl.multiple_of(16 * of, 16), 16)

    with jax.named_scope("scatter"):
        for t in range(1, 8):
            to = lax.rem(m + t, 8)
            send(None, half.at[:, lines(to)], pieces.at[t - 1],
                 rs_send.at[t - 1], rs_sem.at[t - 1],
                 device(x, 2 * (to % 2) + y_lo, to // 2, c))
        lax.fori_loop(0, 64, sent, 0)
        total = half[:, lines(m), :]
        for t in range(1, 8):
            arrived(pieces.at[t - 1], rs_sem.at[t - 1])
            total = total + pieces[t - 1]
        whole[c, :, lines(m), :] = total * (1.0 / NG)
    with jax.named_scope("spread"):
        def share(core, of, s_sem, target):
            ref = whole.at[core, :, lines(of)]
            send(None, ref, ref, s_sem, ag_sem.at[core * 8 + of], target)

        for t in range(1, 8):
            to = lax.rem(m + t, 8)
            share(c, m, ag_send.at[t - 1], device(x, 2 * (to % 2) + y_lo, to // 2, c))
        share(c, m, ag_cross.at[0], device(x, y, z, 1 - c))
        for row in range(4):
            for part_no in range(2):
                block = ys.at[2 * (2 * xs(row // 2) + row % 2) + part_no]
                sem = y_send.at[2 * row + part_no]
                if row < 2:
                    arrived(block, sem)
                else:
                    pl.when(jnp.logical_not(outer))(lambda: arrived(block, sem))
                pl.when(place != row)(lambda: arrived(block, own_send.at[2 * row + part_no]))
        for t in range(1, 8):
            of = lax.rem(m + 8 - t, 8)
            arrived(whole.at[c, :, lines(of)], ag_sem.at[c * 8 + of])
            share(c, of, ag_cross.at[t], device(x, y, z, 1 - c))
        for of in range(8):
            arrived(whole.at[1 - c, :, lines(of)], ag_sem.at[(1 - c) * 8 + of])
        at = 0
        for r in range(4):
            for s in range(r + 1):
                block = whole[at // 5, at % 5]
                inter[128 * r : 128 * r + 128, 128 * s : 128 * s + 128] = block
                if s < r:
                    inter[128 * s : 128 * s + 128, 128 * r : 128 * r + 128] = block.T
                at += 1
    finish_sends()
    for write in writes:
        write.wait()


def local(psi, lower):
    dma = pltpu.SemaphoreType.DMA
    out, inter = pl.pallas_call(
        kernel,
        out_shape=(
            pltpu.VMEM((512, 512), F32),
            pltpu.VMEM((512, 512), F32),
        ),
        in_specs=[pl.BlockSpec(memory_space=pl.ANY)] * 2,
        out_specs=(pl.BlockSpec(memory_space=pltpu.VMEM),) * 2,
        scratch_shapes=[
            pltpu.VMEM((80, 256, 256), F32),
            pltpu.VMEM((16, 256, 128), F32),
            pltpu.VMEM((4, 512, 128), F32),
            pltpu.VMEM((4, 2, 256, 128), F32),
            pltpu.VMEM((10, 128, 128), F32),
            pltpu.VMEM((5, 128, 128), F32),
            pltpu.VMEM((7, 5, 16, 128), F32),
            pltpu.VMEM((2, 5, 128, 128), F32),
            pltpu.VMEM((256, 256), F32),
            dma((80,)), dma((40,)), dma((4,)), dma((4,)),
            dma((16,)), dma((8,)), dma((4, 2)), dma((8,)), dma((2,)), dma((7,)), dma((7,)),
            dma((16,)), dma((7,)), dma((8,)), dma((12,)),
        ],
        compiler_params=pltpu.CompilerParams(
            has_side_effects=True, collective_id=0, vmem_limit_bytes=60 * 1024 * 1024
        ),
    )(psi, lower)
    return out, inter


def solution(mesh):
    return jax.shard_map(
        local,
        mesh=mesh,
        in_specs=(P("band", "ga"), P("band", "ga")),
        out_specs=(P("band", "ga"), P("band", None)),
        check_vma=False,
    )
```

```python
import jax
import jax.numpy as jnp
from jax import lax
from jax.experimental import pallas as pl
from jax.experimental.pallas import tpu as pltpu
from jax.sharding import PartitionSpec as P

MESH = pl.DeviceIdType.MESH
F32 = jnp.float32
BF16 = jnp.bfloat16
NG = 8192

EVENTS = (
    (35402841, 403997254, 191693791, 239968919, 511824708, 362898593, 834718300,
     948628116, 849059307, 663669747, 1072426413, 1016552763, 2365),
    (102506776, 174338574, 438589328, 523088850, 558155168, 685864796, 816289043,
     576168810, 602917612, 634379185, 1066659122, 664493037, 3511),
    (538452489, 273027523, 675118633, 962912907, 206143827, 602649430, 806557866,
     447608085, 1016481691, 768200556, 668198771, 802581439, 3511),
    (56754690, 68556361, 102539994, 642103824, 227093068, 328117276, 666520271,
     836365277, 626060117, 931110444, 845129139, 886570750, 3901),
    (31598824, 143658601, 720046449, 101519049, 35595371, 754398439, 1012818578,
     255513304, 336698646, 1062600622, 439375797, 930308975, 1883),
    (25848384, 86145256, 814758808, 78270635, 182033393, 152857754, 313854771,
     493735544, 215293387, 1073431443, 351250398, 1012495189, 1021),
    (392429635, 463831561, 322577128, 597469575, 488182769, 96596804, 380458138,
     791909378, 514516792, 848509268, 1052209146, 1039096631, 3388),
    (135798785, 940339470, 589965829, 304936633, 270947928, 464045481, 474339643,
     339113978, 398584235, 1011817261, 365882557, 920080382, 3063),
)
SHARE_AT = (13, 13, 41, 34, 35, 44, 15, 15)
STAGE_AT = (38, 42, 52, 56, 62, 62, 51, 61)
EVENT_COUNT = (62, 62, 62, 62, 62, 62, 62, 62)
BY_PAIR = ((51726, 51726), (526, 526), (32510, 32510), (14, 14))
BOTH_WAYS = ((2, 2), (1, 1), (3, 3), (2, 2))


def split(a):
    high = a.astype(BF16)
    return high, (a - high.astype(F32)).astype(BF16)


def product(a, b):
    ah, al = split(a)
    bh, bl = split(b)

    def dot(p, q):
        return jnp.dot(p, q, preferred_element_type=F32)

    return dot(ah, bh) + (dot(ah, bl) + dot(al, bh))


def outer_product(a, b):
    ah, al = split(a)
    bh, bl = split(b)

    def dot(p, q):
        return lax.dot_general(p, q, (((1,), (1,)), ((), ())), preferred_element_type=F32)

    return dot(ah, bl) + dot(
        jnp.concatenate([ah, al], axis=1), jnp.concatenate([bh, bh], axis=1)
    )


def narrow_product(a, b):
    ah, al = split(a)
    bh, bl = split(b)
    wide = jnp.dot(ah, jnp.concatenate([bh, bl], axis=1), preferred_element_type=F32)
    rest = jnp.dot(al, bh, preferred_element_type=F32)
    return wide[:, :128] + (wide[:, 128:] + rest)


def kernel(
    psi, lower, out, inter,
    tiles, ys, rhs, owned, part, half, pieces, whole, inverse,
    tile_sem, quarter_send, rhs_sem, rhs_send,
    y_sem, y_send, own_sem, own_send, half_sem, rs_sem, rs_send, ag_sem, ag_send,
    ag_cross, local_sem,
):
    band = lax.axis_index("band")
    ga = lax.axis_index("ga")
    x, y_lo = band // 2, band % 2
    z, y_hi, c = ga // 4, (ga // 2) % 2, ga % 2
    y = 2 * y_hi + y_lo
    h_own = x // 2
    outer = jnp.logical_or(x == 0, x == 3)
    x_low = jnp.minimum(x, 3 - x)
    place = 2 * h_own + y_lo

    def device(dx, dy, dz, dc):
        return (2 * dx + dy % 2, 4 * dz + 2 * (dy // 2) + dc)

    def xs(h):
        return x_low * (1 - h) + (3 - x_low) * h

    low, high = 2 * x_low, 2 * (3 - x_low)

    def slot(row, j, a, b):
        before = jnp.where(row > 0, low + 1, 0) + jnp.where(row > 1, low + 2, 0)
        before = before + jnp.where(row > 2, high + 1, 0)
        return ((before + j) * 2 + a) * 2 + b

    pending = []

    def send(cond, src, dst, s_sem, r_sem, target, later=True):
        copy = pltpu.make_async_remote_copy(
            src_ref=src, dst_ref=dst, send_sem=s_sem, recv_sem=r_sem,
            device_id=target, device_id_type=MESH,
        )
        if cond is None:
            copy.start()
        else:
            pl.when(cond)(copy.start)
        if later:
            pending.append((cond, copy))
        return copy

    def arrived(ref, sem):
        pltpu.make_async_copy(ref, ref, sem).wait()

    j_own = 2 * z + y_hi
    loads = []
    for a in range(2):
        load = pltpu.make_async_copy(
            lower.at[256 * a : 256 * a + 256, :], tiles.at[slot(place, j_own, a, c)],
            local_sem.at[1 + a],
        )
        needed = 2 * j_own + c <= 2 * band + a
        pl.when(needed)(load.start)
        loads.append((needed, load))
    psi_here = pltpu.make_async_copy(
        psi.at[:, pl.ds(pl.multiple_of(128 * place, 128), 128)], rhs.at[place], local_sem.at[0]
    )
    psi_here.start()

    def place_of(v):
        return lax.rem(v + 8, 4)

    barrier = pltpu.get_barrier_semaphore()
    friends = [
        (3 - x, y, z, c), (x, 2 * y_hi + 1 - y_lo, z, c), (3 - x, 2 * y_hi + 1 - y_lo, z, c),
        (x + 1 - 2 * (x % 2), y, z, c), (x, y, z, 1 - c),
        (x, place_of(y + 1), z, c), (x, place_of(y - 1), z, c),
        (x, y, place_of(z + 1), c), (x, y, place_of(z - 1), c),
    ] + [
        (x, 2 * (lax.rem(j_own + t, 8) % 2) + y_lo, lax.rem(j_own + t, 8) // 2, c)
        for t in range(1, 8)
    ]
    for friend in friends:
        pl.semaphore_signal(barrier, inc=1, device_id=device(*friend), device_id_type=MESH)
    pl.semaphore_wait(barrier, len(friends))
    for needed, load in loads:
        pl.when(needed)(load.wait)

    def quarter(h, a, k, s):
        sgn = 1 - 2 * a
        yo = place_of(y - sgn * (k * c + s * (1 - c)))
        zo = place_of(z - sgn * (k * (1 - c) + s * c))
        row, j = 2 * h + yo % 2, 2 * zo + yo // 2
        i = 2 * xs(h) + yo % 2
        here = slot(row, j, a, c)
        return here, 2 * j + c <= 2 * i + a

    diagonal = j_own == band

    def both(*conds):
        out = conds[0]
        for cond in conds[1:]:
            out = jnp.logical_and(out, cond)
        return out

    def role(values, h):
        of = [jnp.where(c == 0, jnp.int32(a), jnp.int32(b)) for a, b in values]
        return jnp.where(
            outer, jnp.where(h == 0, of[2], of[3]), jnp.where(h == 0, of[0], of[1])
        )

    def by_pair(h, k, s):
        return lax.shift_right_logical(role(BY_PAIR, h), 4 * k + s) % 2 == 1

    def both_ways(h, along_y):
        return lax.shift_right_logical(role(BOTH_WAYS, h), along_y) % 2 == 1

    def copies(h, a, k, s):
        here, real = quarter(h, a, k, s)
        sgn = 1 - 2 * a
        ours = h == h_own
        short1, short2 = both_ways(h, c), both_ways(h, 1 - c)
        ref = tiles.at[here]

        def along(m):
            return device(x, place_of(y + m * c), place_of(z + m * (1 - c)), c)

        def over(m):
            return device(x, place_of(y + m * (1 - c)), place_of(z + m * c), c)

        def ring(k2, s2):
            return both(real, jnp.logical_or(ours, jnp.logical_not(by_pair(h, k2, s2))))

        last1 = 3 - short1.astype(jnp.int32)
        last2 = 3 - short2.astype(jnp.int32)
        near = both(k == 0, s == 0)
        plan = (
            (both(real, ours, jnp.logical_or(near, by_pair(h, k, s))), device(3 - x, y, z, c)),
            (both(ring(k + 1, 0), s == 0, k < last1), along(sgn)),
            (both(ring(3, 0), near, short1), along(-sgn)),
            (both(ring(k, s + 1), s < last2), over(sgn)),
            (both(ring(k, 3), s == 0, short2), over(-sgn)),
            (real, device(x, y, z, 1 - c)),
        )
        sem = quarter_send.at[here // 2]
        return sem, [
            (cond, pltpu.make_async_remote_copy(
                src_ref=ref, dst_ref=ref, send_sem=sem, recv_sem=tile_sem.at[here],
                device_id=target, device_id_type=MESH,
            ))
            for cond, target in plan
        ]

    def finish_sends():
        for cond, copy in pending:
            if cond is None:
                copy.wait_send()
            else:
                pl.when(cond)(copy.wait_send)
        pending.clear()

    def own_quarters(ready):
        for a in range(2):
            for cond, copy in copies(h_own, a, 0, 0)[1]:
                pl.when(both(cond, ready(a)))(copy.start)

    def decode(code):
        return code // 32, code % 2, (code // 8) % 4, (code // 2) % 4

    kind = 2 * x + c

    def by_kind(values):
        out = jnp.int32(values[0])
        for n, value in enumerate(values[1:]):
            out = jnp.where(kind == n + 1, jnp.int32(value), out)
        return out

    words = [by_kind(word) for word in zip(*EVENTS)]

    def event(n, carry):
        which = n // 5
        word = words[0]
        for at, other in enumerate(words[1:]):
            word = jnp.where(which == at + 1, other, word)
        h, a, k, s = decode(lax.shift_right_logical(word, 6 * (n % 5)) % 64)
        here, real = quarter(h, a, k, s)
        pl.when(both(real, jnp.logical_not(both(h == h_own, k == 0, s == 0))))(
            lambda: arrived(tiles.at[here], tile_sem.at[here])
        )
        for cond, copy in copies(h, a, k, s)[1]:
            pl.when(cond)(copy.start)
        return carry

    def sent(code, carry):
        sem, sends = copies(*decode(code))
        number = sum(cond.astype(jnp.int32) for cond, _ in sends)
        for n in range(1, 7):
            pl.when(number == n)(lambda: arrived(tiles.at[pl.ds(0, n)], sem))
        return carry

    own_quarters(lambda a: jnp.logical_not(both(diagonal, c == a)))

    @pl.when(diagonal)
    def _():
        where = slot(place, j_own, c, c)
        rows = lax.broadcasted_iota(jnp.int32, (256, 256), 0)
        cols = lax.broadcasted_iota(jnp.int32, (256, 256), 1)
        tri = tiles[where]
        diag = jnp.where(rows == cols, tri, 0.0)
        down = 1.0 / jnp.sum(diag, axis=1, keepdims=True)
        across = 1.0 / jnp.sum(diag, axis=0, keepdims=True)
        pairs = jnp.logical_and(rows == cols + 1, rows % 2 == 1)
        inverse[...] = jnp.where(rows == cols, down, 0.0) - jnp.where(
            pairs, tri * down * across, 0.0
        )

        def level(k, carry):
            rk, ck = rows >> k, cols >> k
            inside = jnp.logical_and(rk == ck + 1, rk % 2 == 1)
            below = jnp.where(inside, tiles[where], 0.0)
            now = inverse[...]
            inverse[...] = now - product(now, product(below, now))
            return carry

        lax.fori_loop(1, 8, level, 0)
        tiles[where] = inverse[...]

    own_quarters(lambda a: both(diagonal, c == a))

    def share_rhs(when):
        for q in range(4):
            send(
                jnp.logical_and(place != q, when),
                psi.at[:, 128 * q : 128 * q + 128], rhs.at[place],
                rhs_send.at[q], rhs_sem.at[place],
                device(xs(q // 2), 2 * y_hi + q % 2, z, c),
            )

    def tile(row, j, a, b):
        return tiles[slot(row, j, a, b)]

    def from_sibling(row, j, a):
        here = slot(row, j, a, 1 - c)
        arrived(tiles.at[here], tile_sem.at[here])

    def update(row, j):
        for a in range(2):
            from_sibling(row, j, a)
        top, bottom = ys[2 * j], ys[2 * j + 1]
        for a in range(2):
            rhs[row, 256 * a : 256 * a + 256, :] = rhs[row, 256 * a : 256 * a + 256, :] - (
                narrow_product(tile(row, j, a, 0), top) + narrow_product(tile(row, j, a, 1), bottom)
            )

    def deliver(h, r, part_no):
        row = 2 * h + r
        i = 2 * xs(h) + r
        block = ys.at[2 * i + part_no]
        send(None if h == 0 else jnp.logical_not(outer), block, block,
             y_send.at[2 * row + part_no], y_sem.at[2 * i + part_no],
             device(x + 1 - 2 * (x % 2), y, z, c), False)
        send(place != row, block, owned.at[place, part_no], own_send.at[2 * row + part_no],
             own_sem.at[place, part_no], device(xs(h), 2 * y_hi + r, z, c), False)

        @pl.when(place == row)
        def _():
            owned[row, part_no] = ys[2 * i + part_no]

    def solve(h, r):
        row = 2 * h + r
        i = 2 * xs(h) + r

        @pl.when(c == 0)
        def _():
            from_sibling(row, i, 1)

        @pl.when(c == 1)
        def _():
            from_sibling(row, i, 0)
            from_sibling(row, i, 1)

        top = narrow_product(tile(row, i, 0, 0), rhs[row, 0:256, :])
        ys[2 * i] = top
        deliver(h, r, 0)
        bottom = narrow_product(
            tile(row, i, 1, 1), rhs[row, 256:512, :] - narrow_product(tile(row, i, 1, 0), top)
        )
        ys[2 * i + 1] = bottom
        deliver(h, r, 1)

    def await_rhs(h):
        for r in range(2):
            row = 2 * h + r

            @pl.when(place != row)
            def _():
                arrived(rhs.at[row], rhs_sem.at[row])

            @pl.when(place == row)
            def _():
                psi_here.wait()

    def await_y(j):
        for part_no in range(2):
            arrived(ys.at[2 * j + part_no], y_sem.at[2 * j + part_no])

    def by_columns(h, arriving):
        count = 2 * xs(h)

        def step(j, carry):
            pl.when(arriving(j))(lambda: await_y(j))
            update(2 * h, j)
            update(2 * h + 1, j)
            return carry

        lax.fori_loop(0, count, step, 0)
        solve(h, 0)
        update(2 * h + 1, count)
        solve(h, 1)

    def by_rows(h):
        count = 2 * xs(h)
        for r in range(2):
            def step(j, carry, r=r):
                update(2 * h + r, j)
                return carry

            lax.fori_loop(0, count + r, step, 0)
            solve(h, r)

    share_at, stage_at, count = by_kind(SHARE_AT), by_kind(STAGE_AT), by_kind(EVENT_COUNT)
    share_rhs(h_own == 0)
    with jax.named_scope("first"):
        lax.fori_loop(0, share_at, event, 0)
    share_rhs(h_own == 1)
    with jax.named_scope("second"):
        lax.fori_loop(share_at, stage_at, event, 0)
    with jax.named_scope("early"):
        await_rhs(0)
        by_columns(0, lambda j: jnp.logical_not(outer))
    with jax.named_scope("third"):
        lax.fori_loop(stage_at, count, event, 0)
    with jax.named_scope("last"):
        await_rhs(1)

        @pl.when(outer)
        def _():
            by_columns(1, lambda j: j >= 2)

        @pl.when(jnp.logical_not(outer))
        def _():
            by_rows(1)

    writes = []
    with jax.named_scope("product"):
        beside = place + 1 - 2 * (place % 2)
        for n, q in enumerate(
            (place, beside, lax.rem(place + 2, 4), lax.rem(beside + 2, 4))
        ):
            for a in range(2):
                if n:
                    arrived(owned.at[q, a], own_sem.at[q, a])
                write = pltpu.make_async_copy(
                    owned.at[q, a],
                    out.at[
                        256 * a : 256 * a + 256, pl.ds(pl.multiple_of(128 * q, 128), 128)
                    ],
                    local_sem.at[3 + 2 * n + a],
                )
                write.start()
                writes.append(write)
            block = owned[q].reshape(512, 128)
            at = 0
            for r in range(4):
                term = outer_product(
                    block[128 * r : 128 * r + 128], block[: 128 * r + 128]
                )
                for s in range(r + 1):
                    here = term[:, 128 * s : 128 * s + 128]
                    part[at] = here if n == 0 else part[at] + here
                    at += 1

    with jax.named_scope("halves"):
        send(None, part.at[pl.ds(5 - 5 * c, 5)], half, half_sem.at[0], half_sem.at[1],
             device(x, y, z, 1 - c))
        arrived(half, half_sem.at[1])
        half[...] = half[...] + part[pl.ds(5 * c, 5)]
    m = j_own

    def lines(of):
        return pl.ds(pl.multiple_of(16 * of, 16), 16)

    with jax.named_scope("scatter"):
        for t in range(1, 8):
            to = lax.rem(m + t, 8)
            send(None, half.at[:, lines(to)], pieces.at[t - 1],
                 rs_send.at[t - 1], rs_sem.at[t - 1],
                 device(x, 2 * (to % 2) + y_lo, to // 2, c))
        lax.fori_loop(0, 64, sent, 0)
        finish_sends()
        for write in writes:
            write.wait()
        total = half[:, lines(m), :]
        for t in range(1, 8):
            arrived(pieces.at[t - 1], rs_sem.at[t - 1])
            total = total + pieces[t - 1]
        whole[c, :, lines(m), :] = total * (1.0 / NG)
    with jax.named_scope("spread"):
        def share(core, of, s_sem, target):
            ref = whole.at[core, :, lines(of)]
            send(None, ref, ref, s_sem, ag_sem.at[core * 8 + of], target)

        for t in range(1, 8):
            to = lax.rem(m + t, 8)
            share(c, m, ag_send.at[t - 1], device(x, 2 * (to % 2) + y_lo, to // 2, c))
        share(c, m, ag_cross.at[0], device(x, y, z, 1 - c))
        for row in range(4):
            for part_no in range(2):
                block = ys.at[2 * (2 * xs(row // 2) + row % 2) + part_no]
                sem = y_send.at[2 * row + part_no]
                if row < 2:
                    arrived(block, sem)
                else:
                    pl.when(jnp.logical_not(outer))(lambda: arrived(block, sem))
                pl.when(place != row)(lambda: arrived(block, own_send.at[2 * row + part_no]))
        for t in range(1, 8):
            of = lax.rem(m + 8 - t, 8)
            arrived(whole.at[c, :, lines(of)], ag_sem.at[c * 8 + of])
            share(c, of, ag_cross.at[t], device(x, y, z, 1 - c))
        for of in range(8):
            arrived(whole.at[1 - c, :, lines(of)], ag_sem.at[(1 - c) * 8 + of])
        at = 0
        for r in range(4):
            for s in range(r + 1):
                block = whole[at // 5, at % 5]
                inter[128 * r : 128 * r + 128, 128 * s : 128 * s + 128] = block
                if s < r:
                    inter[128 * s : 128 * s + 128, 128 * r : 128 * r + 128] = block.T
                at += 1
    finish_sends()


def local(psi, lower):
    dma = pltpu.SemaphoreType.DMA
    out, inter = pl.pallas_call(
        kernel,
        out_shape=(
            pltpu.VMEM((512, 512), F32),
            pltpu.VMEM((512, 512), F32),
        ),
        in_specs=[pl.BlockSpec(memory_space=pl.ANY)] * 2,
        out_specs=(pl.BlockSpec(memory_space=pltpu.VMEM),) * 2,
        scratch_shapes=[
            pltpu.VMEM((80, 256, 256), F32),
            pltpu.VMEM((16, 256, 128), F32),
            pltpu.VMEM((4, 512, 128), F32),
            pltpu.VMEM((4, 2, 256, 128), F32),
            pltpu.VMEM((10, 128, 128), F32),
            pltpu.VMEM((5, 128, 128), F32),
            pltpu.VMEM((7, 5, 16, 128), F32),
            pltpu.VMEM((2, 5, 128, 128), F32),
            pltpu.VMEM((256, 256), F32),
            dma((80,)), dma((40,)), dma((4,)), dma((4,)),
            dma((16,)), dma((8,)), dma((4, 2)), dma((8,)), dma((2,)), dma((7,)), dma((7,)),
            dma((16,)), dma((7,)), dma((8,)), dma((12,)),
        ],
        compiler_params=pltpu.CompilerParams(
            has_side_effects=True, collective_id=0, vmem_limit_bytes=60 * 1024 * 1024
        ),
    )(psi, lower)
    return out, inter


def solution(mesh):
    return jax.shard_map(
        local,
        mesh=mesh,
        in_specs=(P("band", "ga"), P("band", "ga")),
        out_specs=(P("band", "ga"), P("band", None)),
        check_vma=False,
    )
```
